256 devices in a mesh: dp: 32 (over z, x_lo, core), expert: 8 (over x_hi, y).
Axes of the slice: x: 4 (x_hi: 2, x_lo: 2; x = x_hi * 2 + x_lo), y: 4, z: 8, core: 2. Of those that a mesh axis runs over, the one named last changes fastest.
Arguments:
- stash: bfloat16 [32768, 6144], P(('dp', 'expert')), may hold values from -24 to 24
- scales: bfloat16 [32768, 48], P(('dp', 'expert')), may hold values from 0.099609375 to 2
- out_grad: bfloat16 [32768, 6144], P(('dp', 'expert')), may hold values from -6 to 6
- route_ids: int32 [32768, 2], P(('dp', 'expert')), may hold values from 0 to 7, as said below
- gates: float32 [32768, 2], P(('dp', 'expert')), may hold values from 0.1 to 1
- w_gate_up: bfloat16 [8, 6144, 512], P('expert'), may hold values from -0.15625 to 0.15625
- w_down: bfloat16 [8, 6144, 256], P('expert', 'dp'), may hold values from -0.078125 to 0.078125
Outputs:
- input_grad: bfloat16 [32768, 6144], P(('dp', 'expert'))
- grad_gate_up: float32 [8, 6144, 512], P('expert', 'dp')
The draws below stay inside these ranges and needn't reach their ends.
Inputs may be any that keep to these rules, and one draw needn't show every extreme that they name: `route_ids`: each token names two different experts. Within each aligned block of 128 tokens no expert is named more than 56 times. In every run of 8 aligned blocks that starts at a multiple of 8 blocks, some expert is named exactly 56 times in each block of the run.
All inputs are finite; a program needn't handle non-finite values.
Results may differ from the reference program's by a relative error of at most 0.023.
Values may be sent and summed in bfloat16 or wider, within the bound.
A program may use at most 128 MiB of HBM per device.

```python
import math
import jax
import jax.numpy as jnp
from jax import lax

D = 6144
HID = 256
QBLK = 128
TOK_DEV = 128
EXPERTS = 8
CAP = 56
TOKENS = 32768
N_DP = 32
N_EXPERT = 8


def device_routes(device_key, hot_expert):
    key_second, key_count, key_perm, key_flip = jax.random.split(device_key, 4)
    slot_total = 2 * TOK_DEV
    second_expert = (hot_expert + jax.random.randint(key_second, (), 1, EXPERTS)) % EXPERTS
    lowest = max(0, slot_total - CAP - (EXPERTS - 2) * CAP)
    highest = min(CAP, slot_total - CAP)
    second_count = jax.random.randint(key_count, (), lowest, highest + 1)
    offsets = jnp.arange(1, EXPERTS, dtype=jnp.int32)
    candidates = (hot_expert + offsets) % EXPERTS
    order_key = jnp.where(candidates == second_expert, EXPERTS, 0) + offsets
    others = candidates[jnp.argsort(order_key)]
    spread = max(EXPERTS - 2, 1)
    places = jnp.arange(slot_total, dtype=jnp.int32)
    rest_index = jnp.maximum(places - CAP - second_count, 0) % spread
    labels = jnp.where(places < CAP, hot_expert, jnp.where(places < CAP + second_count, second_expert, others[rest_index]))
    labels = jnp.sort(labels)
    paired = jnp.stack([labels[:TOK_DEV], labels[TOK_DEV:]], axis=1)
    paired = paired[jax.random.permutation(key_perm, TOK_DEV)]
    flipped = jax.random.randint(key_flip, (TOK_DEV, 1), 0, 2)
    paired = jnp.where(flipped == 1, paired[:, ::-1], paired)
    return paired.astype(jnp.int32)


def draw_route_ids(key, part):
    base_key = jax.random.fold_in(key, 7)
    key_hot, key_devices = jax.random.split(base_key)
    hot_rows = jax.random.randint(key_hot, (N_DP,), 0, EXPERTS)
    hot_devices = jnp.repeat(hot_rows, N_EXPERT)
    device_keys = jax.random.split(key_devices, N_DP * N_EXPERT)
    paired = jax.vmap(device_routes)(device_keys, hot_devices)
    return paired.reshape(TOKENS, 2).astype(jnp.int32)


def with_spikes(result, own_key, source, target, blocks, factor):
    owner, partner = [(jnp.arange(result.shape[dim]) // (result.shape[dim] // blocks)).reshape([-1 if axis == dim else 1 for axis in range(result.ndim)]) for dim in (source, target)]
    chosen = jax.random.permutation(own_key, blocks)[partner]
    strong = (owner == chosen) | (owner == (partner + blocks // 2) % blocks)
    return jnp.where(strong, factor * result, result)


def block_scale(stream_key, shape, pieces, low, largest):
    level = 1.0
    for position, blocks in pieces:
        steps = jax.random.uniform(jax.random.fold_in(jax.random.fold_in(stream_key, 6), position), (blocks,), jnp.float32, low / len(pieces), largest / len(pieces))
        level = level * jnp.repeat(jnp.exp(steps), shape[position] // blocks).reshape((-1,) + (1,) * (len(shape) - 1 - position))
    return level


def noise(key, shape, scale, bound, pieces=(), kind=jnp.bfloat16):
    result = jax.random.normal(key, shape, jnp.float32) * scale
    if len(pieces) > 0:
        result = block_scale(key, shape, pieces, -0.22, 0.18) * result
    return jnp.clip(result, min=-bound, max=bound).astype(kind)


def noise_with(own_key, shape, width, reach, cuts, heavy, held_as=jnp.bfloat16):
    entries = width * jax.random.normal(own_key, shape, jnp.float32)
    if cuts:
        entries = entries * block_scale(own_key, shape, cuts, -0.22, 0.18)
    return jnp.clip(with_spikes(entries, jax.random.fold_in(own_key, 3), *heavy), -reach, reach).astype(held_as)


def setup_inputs(seed: int = 0) -> dict:
    arg_keys = jax.random.split(jax.random.key(seed), 8)
    stash = noise_with(arg_keys[0], (TOKENS, D), 1.0, 24.0, ((0, 256),), (0, 1, 256, 6.0))
    scales = jnp.clip(jnp.exp(math.log(2.0) - 2.9996462 * jax.random.uniform(arg_keys[1], (TOKENS, D // QBLK), jnp.float32) ** block_scale(arg_keys[1], (TOKENS, D // QBLK), ((0, 256),), -0.2, 0.2)), 0.099609375, 2.0).astype(jnp.bfloat16)
    out_grad = noise(arg_keys[2], (TOKENS, D), 1.0, 6.0, ((0, 256),))
    route_ids = draw_route_ids(jax.random.fold_in(arg_keys[7], 71), 0)
    gates = jnp.clip(0.1 + 0.9 * jax.random.uniform(arg_keys[4], (TOKENS, 2), jnp.float32) ** block_scale(arg_keys[4], (TOKENS, 2), ((0, 256),), -0.2, 0.2), 0.1, 1.0)
    w_gate_up = noise(arg_keys[5], (EXPERTS, D, 2 * HID), (D // 4) ** -0.5, 0.15625, ((0, 8),))
    w_down = noise(arg_keys[6], (EXPERTS, D, HID), D ** -0.5, 0.078125, ((0, 8), (1, 32)))
    return {"stash": stash, "scales": scales, "out_grad": out_grad, "route_ids": route_ids, "gates": gates, "w_gate_up": w_gate_up, "w_down": w_down}


def dispatch_plan(route_ids):
    flat_ids = route_ids.reshape(-1).astype(jnp.int32)
    onehot = (flat_ids[:, None] == jnp.arange(EXPERTS, dtype=jnp.int32)[None, :]).astype(jnp.int32)
    earlier = (jnp.cumsum(onehot, axis=0) - onehot).astype(jnp.int32)
    ranking = jnp.sum(earlier * onehot, axis=1).astype(jnp.int32)
    destination = (flat_ids * CAP + ranking).astype(jnp.int32)
    slot_total = 2 * TOK_DEV
    source = jnp.full((EXPERTS * CAP,), slot_total, jnp.int32)
    source = source.at[destination].set(jnp.arange(slot_total, dtype=jnp.int32))
    return destination, source


def source_side(stash, scales, out_grad, route_ids, gates):
    destination, source = dispatch_plan(route_ids)
    slot_total = 2 * TOK_DEV
    live_rows = (source < slot_total)[:, None]
    token_index = jnp.minimum(source // 2, TOK_DEV - 1).astype(jnp.int32)
    slot_index = jnp.minimum(source, slot_total - 1).astype(jnp.int32)
    sent_stash = jnp.where(live_rows, stash[token_index], jnp.zeros((), stash.dtype))
    sent_scale = jnp.where(live_rows, scales[token_index], jnp.zeros((), scales.dtype))
    weighted = gates.reshape(-1)[slot_index][:, None] * out_grad[token_index].astype(jnp.float32)
    sent_grad = jnp.where(live_rows, weighted, jnp.zeros((), jnp.float32)).astype(jnp.bfloat16)
    return (sent_stash.reshape(EXPERTS, CAP, D), sent_scale.reshape(EXPERTS, CAP, D // QBLK),
            sent_grad.reshape(EXPERTS, CAP, D), destination)


def dequantize(stash_rows, scale_rows):
    row_total = stash_rows.shape[0]
    blocks = scale_rows.shape[1]
    scaled = stash_rows.reshape(row_total, blocks, -1).astype(jnp.float32) * scale_rows.astype(jnp.float32)[:, :, None]
    return scaled.reshape(row_total, -1).astype(jnp.bfloat16)


def gated_backward(gate_up, back_hidden):
    hidden = back_hidden.shape[1]
    gate_value = gate_up[:, :hidden]
    up_value = gate_up[:, hidden:]
    sigmoid_gate = jax.nn.sigmoid(gate_value)
    grad_gate = back_hidden * up_value * sigmoid_gate * (1.0 + gate_value * (1.0 - sigmoid_gate))
    grad_up = back_hidden * gate_value * sigmoid_gate
    return jnp.concatenate([grad_gate, grad_up], axis=1).astype(jnp.bfloat16)


def expert_pass(inputs):
    got_stash, got_scale, got_grad, weight_in, weight_out = inputs
    row_total = got_stash.shape[0] * got_stash.shape[1]
    features = dequantize(got_stash.reshape(row_total, D), got_scale.reshape(row_total, -1))
    gate_up = jnp.dot(features, weight_in, preferred_element_type=jnp.float32)
    upstream = got_grad.reshape(row_total, D)
    back_hidden = jnp.dot(upstream, weight_out, preferred_element_type=jnp.float32)
    hidden_grad = gated_backward(gate_up, back_hidden)
    slot_grads = lax.dot_general(hidden_grad, weight_in, (((1,), (1,)), ((), ())),
                                 preferred_element_type=jnp.float32).astype(jnp.bfloat16)
    partial_grad = lax.dot_general(features, hidden_grad, (((0,), (0,)), ((), ())),
                                   preferred_element_type=jnp.float32)
    return slot_grads, partial_grad


def combine_slots(returned, destination):
    picked = returned[destination].astype(jnp.float32).reshape(TOK_DEV, 2, D)
    return jnp.sum(picked, axis=1).astype(jnp.bfloat16)


def reference(stash, scales, out_grad, route_ids, gates, w_gate_up, w_down):
    blocks = D // QBLK
    stacked = (stash.reshape(N_DP, N_EXPERT, TOK_DEV, D),
               scales.reshape(N_DP, N_EXPERT, TOK_DEV, blocks),
               out_grad.reshape(N_DP, N_EXPERT, TOK_DEV, D),
               route_ids.reshape(N_DP, N_EXPERT, TOK_DEV, 2),
               gates.reshape(N_DP, N_EXPERT, TOK_DEV, 2))

    def row_step(running, row_inputs):
        row_stash, row_scales, row_grad, row_ids, row_gates = row_inputs
        sent_stash, sent_scale, sent_grad, destination = jax.vmap(source_side)(
            row_stash, row_scales, row_grad, row_ids, row_gates)
        received = (jnp.swapaxes(sent_stash, 0, 1), jnp.swapaxes(sent_scale, 0, 1),
                    jnp.swapaxes(sent_grad, 0, 1), w_gate_up, w_down)
        slot_grads, partial_grad = lax.map(expert_pass, received)
        returned = jnp.swapaxes(slot_grads.reshape(EXPERTS, N_EXPERT, CAP, D), 0, 1)
        returned = returned.reshape(N_EXPERT, EXPERTS * CAP, D)
        token_grads = jax.vmap(combine_slots)(returned, destination)
        return running + partial_grad, token_grads

    initial = jnp.zeros((EXPERTS, D, 2 * HID), jnp.float32)
    total_grad, token_grads = lax.scan(row_step, initial, stacked)
    return token_grads.reshape(TOKENS, D), total_grad / N_DP
```

```python
import functools

import jax
import jax.numpy as jnp
from jax import lax
from jax.experimental import pallas as pl
from jax.experimental.pallas import tpu as pltpu
from jax.sharding import PartitionSpec as P

MESH = pl.DeviceIdType.MESH


def ring_place():
    index = lax.axis_index("dp")
    return index // 4, lax.rem(index // 2, 2), lax.rem(index, 2)


def greet(partners):
    barrier = pltpu.get_barrier_semaphore()
    for partner in partners:
        pl.semaphore_signal(barrier, inc=1, device_id={"dp": partner}, device_id_type=MESH)
    pl.semaphore_wait(barrier, len(partners))


def gather_kernel(zs, own_ref, out_ref, local_sem, send_sems, recv_sems):
    z, xlo, core = ring_place()

    def at(zz, xx, cc):
        return zz * 4 + xx * 2 + cc

    up, down = lax.rem(z + 1, zs), lax.rem(z + zs - 1, zs)
    to_up, to_down = at(up, xlo, core), at(down, xlo, core)
    to_side, to_twin = at(z, 1 - xlo, core), at(z, xlo, 1 - core)
    greet((to_up, to_down, to_side, to_twin))
    me = at(z, xlo, core)
    keep = pltpu.make_async_copy(own_ref, out_ref.at[me], local_sem)
    keep.start()
    sends = []
    forward = zs // 2
    backward = zs - 1 - forward

    def send(source, piece, number, target):
        copy = pltpu.make_async_remote_copy(
            src_ref=source,
            dst_ref=out_ref.at[piece],
            send_sem=send_sems.at[number],
            recv_sem=recv_sems.at[number],
            device_id={"dp": target},
            device_id_type=MESH,
        )
        copy.start()
        sends.append(copy)

    def arrive(piece, number):
        pltpu.make_async_remote_copy(
            src_ref=own_ref,
            dst_ref=out_ref.at[piece],
            send_sem=send_sems.at[number],
            recv_sem=recv_sems.at[number],
            device_id={"dp": me},
            device_id_type=MESH,
        ).wait_recv()

    ups, downs, twins = 1, 1 + 2 * forward, 1 + 2 * forward + 2 * backward
    send(own_ref, me, 0, to_side)
    send(own_ref, me, ups, to_up)
    send(own_ref, me, downs, to_down)
    send(own_ref, me, twins, to_twin)
    arrive(to_side, 0)
    send(out_ref.at[to_side], to_side, ups + 1, to_up)
    send(out_ref.at[to_side], to_side, downs + 1, to_down)
    send(out_ref.at[to_side], to_side, twins + 1, to_twin)
    for hop in range(1, forward + 1):
        for pair in range(2):
            xx = xlo if pair == 0 else 1 - xlo
            piece = at(lax.rem(z + zs - hop, zs), xx, core)
            arrive(piece, ups + 2 * (hop - 1) + pair)
            if hop < forward:
                send(out_ref.at[piece], piece, ups + 2 * hop + pair, to_up)
            send(out_ref.at[piece], piece, twins + 2 * hop + pair, to_twin)
            if hop <= backward:
                piece = at(lax.rem(z + hop, zs), xx, core)
                arrive(piece, downs + 2 * (hop - 1) + pair)
                if hop < backward:
                    send(out_ref.at[piece], piece, downs + 2 * hop + pair, to_down)
                send(out_ref.at[piece], piece, twins + 2 * (forward + hop) + pair, to_twin)
    for pair in range(2):
        xx = xlo if pair == 0 else 1 - xlo
        arrive(at(z, xx, 1 - core), twins + pair)
        for hop in range(1, forward + 1):
            arrive(at(lax.rem(z + zs - hop, zs), xx, 1 - core), twins + 2 * hop + pair)
        for hop in range(1, backward + 1):
            arrive(at(lax.rem(z + hop, zs), xx, 1 - core), twins + 2 * (forward + hop) + pair)
    for copy in sends:
        copy.wait_send()
    keep.wait()


def gather_rows(own, dp_count, collective_id):
    zs = dp_count // 4
    copies = 1 + 2 * (zs - 1) + 2 * zs
    return pl.pallas_call(
        functools.partial(gather_kernel, zs),
        out_shape=jax.ShapeDtypeStruct((dp_count,) + own.shape, own.dtype),
        in_specs=[pl.BlockSpec(memory_space=pltpu.VMEM)],
        out_specs=pl.BlockSpec(memory_space=pl.ANY),
        scratch_shapes=[
            pltpu.SemaphoreType.DMA,
            pltpu.SemaphoreType.DMA((copies,)),
            pltpu.SemaphoreType.DMA((copies,)),
        ],
        compiler_params=pltpu.CompilerParams(collective_id=collective_id, has_side_effects=True),
        cost_estimate=pl.CostEstimate(flops=20_000_000_000, bytes_accessed=3_000_000, transcendentals=0),
        name="gather_rows",
    )(own)


def reduce_kernel(zs, subs, part_ref, out_ref, core_ref, ring_ref, stage_ref, side_ref,
                  core_send, core_recv, ring_send, ring_recv, side_send, side_recv):
    z, xlo, core = ring_place()
    rows = part_ref.shape[1]
    step_rows = rows // subs

    def at(zz, xx, cc):
        return zz * 4 + xx * 2 + cc

    up, down = lax.rem(z + 1, zs), lax.rem(z + zs - 1, zs)
    to_up, to_down = at(up, xlo, core), at(down, xlo, core)
    to_side, to_twin = at(z, 1 - xlo, core), at(z, xlo, 1 - core)
    greet((to_up, to_down, to_side, to_twin))

    def owner(way, step):
        return lax.rem(z + 2 * zs - 1 - step, zs) if way == 0 else lax.rem(z + 1 + step, zs)

    def core_copy(way, step):
        piece = owner(way, step)
        return pltpu.make_async_remote_copy(
            src_ref=part_ref.at[at(piece, way, 1 - core)],
            dst_ref=core_ref.at[way, step],
            send_sem=core_send.at[way, step],
            recv_sem=core_recv.at[way, step],
            device_id={"dp": to_twin},
            device_id_type=MESH,
        )

    def ring_copy(way, step, sub):
        return pltpu.make_async_remote_copy(
            src_ref=stage_ref.at[way, step, sub],
            dst_ref=ring_ref.at[way, step, sub],
            send_sem=ring_send.at[way, step, sub],
            recv_sem=ring_recv.at[way, step, sub],
            device_id={"dp": to_up if way == 0 else to_down},
            device_id_type=MESH,
        )

    def side_copy(sub):
        return pltpu.make_async_remote_copy(
            src_ref=stage_ref.at[1 - xlo, zs - 1, sub],
            dst_ref=side_ref.at[sub],
            send_sem=side_send.at[sub],
            recv_sem=side_recv.at[sub],
            device_id={"dp": to_side},
            device_id_type=MESH,
        )

    for step in range(zs):
        for way in range(2):
            core_copy(way, step).start()
    for step in range(zs):
        for sub in range(subs):
            for way in range(2):
                if sub == 0:
                    core_copy(way, step).wait_recv()
                piece = at(owner(way, step), way, core)
                span = pl.ds(sub * step_rows, step_rows)
                value = part_ref[piece, span, :].astype(jnp.float32) + core_ref[way, step, span, :].astype(jnp.float32)
                if step > 0:
                    ring_copy(way, step - 1, sub).wait_recv()
                    value = value + ring_ref[way, step - 1, sub].astype(jnp.float32)
                stage_ref[way, step, sub] = value.astype(stage_ref.dtype)
                if step < zs - 1:
                    ring_copy(way, step, sub).start()
        if step == zs - 1:
            for sub in range(subs):
                side_copy(sub).start()
    share = 1.0 / (4 * zs)
    for sub in range(subs):
        side_copy(sub).wait_recv()
        span = pl.ds(sub * step_rows, step_rows)
        total = stage_ref[xlo, zs - 1, sub].astype(jnp.float32) + side_ref[sub].astype(jnp.float32)
        out_ref[span, :] = total * share
    for step in range(zs):
        for way in range(2):
            core_copy(way, step).wait_send()
            for sub in range(subs):
                if step < zs - 1:
                    ring_copy(way, step, sub).wait_send()
    for sub in range(subs):
        side_copy(sub).wait_send()


def reduce_rows(part, dp_count, collective_id, subs=2):
    zs = dp_count // 4
    width = part.shape[1]
    rows = part.shape[0] // dp_count
    kind = part.dtype
    return pl.pallas_call(
        functools.partial(reduce_kernel, zs, subs),
        out_shape=jax.ShapeDtypeStruct((rows, width), jnp.float32),
        in_specs=[pl.BlockSpec(memory_space=pltpu.VMEM)],
        out_specs=pl.BlockSpec(memory_space=pltpu.VMEM),
        scratch_shapes=[
            pltpu.VMEM((2, zs, rows, width), kind),
            pltpu.VMEM((2, zs - 1, subs, rows // subs, width), kind),
            pltpu.VMEM((2, zs, subs, rows // subs, width), kind),
            pltpu.VMEM((subs, rows // subs, width), kind),
            pltpu.SemaphoreType.DMA((2, zs)),
            pltpu.SemaphoreType.DMA((2, zs)),
            pltpu.SemaphoreType.DMA((2, zs - 1, subs)),
            pltpu.SemaphoreType.DMA((2, zs - 1, subs)),
            pltpu.SemaphoreType.DMA((subs,)),
            pltpu.SemaphoreType.DMA((subs,)),
        ],
        compiler_params=pltpu.CompilerParams(
            collective_id=collective_id, has_side_effects=True, vmem_limit_bytes=32 * 1024 * 1024
        ),
        cost_estimate=pl.CostEstimate(flops=40_000_000_000, bytes_accessed=7_000_000, transcendentals=0),
        name="reduce_rows",
    )(part.reshape(dp_count, rows, width))


def dispatch_masks(route_ids, experts, capacity):
    tokens = route_ids.shape[0]
    flat_ids = route_ids.reshape(-1)
    slot_total = flat_ids.shape[0]
    onehot = flat_ids[:, None] == jnp.arange(experts, dtype=jnp.int32)[None, :]
    order = jnp.arange(slot_total, dtype=jnp.int32)
    before = (order[:, None] > order[None, :]).astype(jnp.bfloat16)
    earlier = jnp.dot(before, onehot.astype(jnp.bfloat16), preferred_element_type=jnp.float32)
    ranking = jnp.sum(jnp.where(onehot, earlier, 0.0), axis=1).astype(jnp.int32)
    destination = (flat_ids * capacity + ranking).reshape(tokens, 2)
    rows = jnp.arange(experts * capacity, dtype=jnp.int32)
    first = rows[:, None] == destination[:, 0][None, :]
    second = rows[:, None] == destination[:, 1][None, :]
    return first, second


def dequantize(stash_rows, scale_rows):
    row_total = stash_rows.shape[0]
    blocks = scale_rows.shape[1]
    scaled = (
        stash_rows.reshape(row_total, blocks, -1).astype(jnp.float32)
        * scale_rows.astype(jnp.float32)[:, :, None]
    )
    return scaled.reshape(row_total, -1).astype(jnp.bfloat16)


def gated_backward(gate_up, back_hidden):
    hidden = back_hidden.shape[1]
    gate_value = gate_up[:, :hidden]
    up_value = gate_up[:, hidden:]
    sigmoid_gate = jax.nn.sigmoid(gate_value)
    grad_gate = back_hidden * up_value * sigmoid_gate * (1.0 + gate_value * (1.0 - sigmoid_gate))
    grad_up = back_hidden * gate_value * sigmoid_gate
    return jnp.concatenate([grad_gate, grad_up], axis=1).astype(jnp.bfloat16)


def exchange(rows, experts, capacity):
    width = rows.shape[1]
    moved = lax.all_to_all(
        rows.reshape(experts, capacity, width), "expert", split_axis=0, concat_axis=0, tiled=True
    )
    return moved.reshape(experts * capacity, width)


def on_device(stash, scales, out_grad, route_ids, gates, w_gate_up, w_down):
    tokens, feature_width = stash.shape
    hidden = w_down.shape[2]
    experts = lax.axis_size("expert")
    dp_count = lax.axis_size("dp")
    capacity = min(tokens, 7 * tokens // (2 * experts))
    first, second = dispatch_masks(route_ids, experts, capacity)
    picks = (first | second).astype(jnp.bfloat16)
    row_gate = jnp.sum(
        jnp.where(first, gates[:, 0][None, :], 0.0) + jnp.where(second, gates[:, 1][None, :], 0.0), axis=1
    )
    sent_x = jnp.dot(picks, dequantize(stash, scales), preferred_element_type=jnp.float32).astype(jnp.bfloat16)
    sent_grad = (
        jnp.dot(picks, out_grad, preferred_element_type=jnp.float32) * row_gate[:, None]
    ).astype(jnp.bfloat16)
    weight_in = w_gate_up[0]
    features = exchange(sent_x, experts, capacity)
    gate_up = jnp.dot(features, weight_in, preferred_element_type=jnp.float32)
    upstream = exchange(sent_grad, experts, capacity)
    weight_out = gather_rows(w_down[0], dp_count, 1).reshape(feature_width, hidden)
    back_hidden = jnp.dot(upstream, weight_out, preferred_element_type=jnp.float32)
    hidden_grad = gated_backward(gate_up, back_hidden)
    slot_grads = lax.dot_general(
        hidden_grad, weight_in, (((1,), (1,)), ((), ())), preferred_element_type=jnp.float32
    ).astype(jnp.bfloat16)
    returned = exchange(slot_grads, experts, capacity)
    input_grad = lax.dot_general(
        picks, returned, (((0,), (0,)), ((), ())), preferred_element_type=jnp.float32
    ).astype(jnp.bfloat16)
    local_rows = feature_width // dp_count
    partial_grad = lax.dot_general(
        features, hidden_grad, (((0,), (0,)), ((), ())), preferred_element_type=jnp.float32
    ).astype(jnp.bfloat16)
    grad_gate_up = reduce_rows(partial_grad, dp_count, 2).reshape(1, local_rows, 2 * hidden)
    return (input_grad, grad_gate_up)


def solution(mesh):
    placed = (
        P(("dp", "expert"), None),
        P(("dp", "expert"), None),
        P(("dp", "expert"), None),
        P(("dp", "expert"), None),
        P(("dp", "expert"), None),
        P("expert", None, None),
        P("expert", "dp", None),
    )
    return jax.shard_map(
        on_device,
        mesh=mesh,
        in_specs=placed,
        out_specs=(P(("dp", "expert"), None), P("expert", "dp", None)),
        check_vma=False,
    )
```

```python
import functools

import jax
import jax.numpy as jnp
from jax import lax
from jax.experimental import pallas as pl
from jax.experimental.pallas import tpu as pltpu
from jax.sharding import Mesh
from jax.sharding import PartitionSpec as P

MESH = pl.DeviceIdType.MESH
COLUMN_AXES = ("z", "xlo", "core")
ROW_AXES = ("xhi", "y")


def ring_place():
    return lax.axis_index("z"), lax.axis_index("xlo"), lax.axis_index("core")


def place(z, xlo, core):
    return {"z": z, "xlo": xlo, "core": core}


def greet(partners):
    barrier = pltpu.get_barrier_semaphore()
    for partner in partners:
        pl.semaphore_signal(barrier, inc=1, device_id=partner, device_id_type=MESH)
    pl.semaphore_wait(barrier, len(partners))


def reduce_kernel(zs, subs, part_ref, out_ref, core_ref, ring_ref, stage_ref, side_ref,
                  core_send, core_recv, ring_send, ring_recv, side_send, side_recv):
    z, xlo, core = ring_place()
    rows = part_ref.shape[1]
    step_rows = rows // subs

    def at(zz, xx, cc):
        return zz * 4 + xx * 2 + cc

    up, down = lax.rem(z + 1, zs), lax.rem(z + zs - 1, zs)
    to_up, to_down = place(up, xlo, core), place(down, xlo, core)
    to_side, to_twin = place(z, 1 - xlo, core), place(z, xlo, 1 - core)
    greet((to_up, to_down, to_side, to_twin))

    def owner(way, step):
        return lax.rem(z + 2 * zs - 1 - step, zs) if way == 0 else lax.rem(z + 1 + step, zs)

    def core_copy(way, step):
        piece = owner(way, step)
        return pltpu.make_async_remote_copy(
            src_ref=part_ref.at[at(piece, way, 1 - core)],
            dst_ref=core_ref.at[way, step],
            send_sem=core_send.at[way, step],
            recv_sem=core_recv.at[way, step],
            device_id=to_twin,
            device_id_type=MESH,
        )

    def ring_copy(way, step, sub):
        return pltpu.make_async_remote_copy(
            src_ref=stage_ref.at[way, step, sub],
            dst_ref=ring_ref.at[way, step, sub],
            send_sem=ring_send.at[way, step, sub],
            recv_sem=ring_recv.at[way, step, sub],
            device_id=to_up if way == 0 else to_down,
            device_id_type=MESH,
        )

    def side_copy(sub):
        return pltpu.make_async_remote_copy(
            src_ref=stage_ref.at[1 - xlo, zs - 1, sub],
            dst_ref=side_ref.at[sub],
            send_sem=side_send.at[sub],
            recv_sem=side_recv.at[sub],
            device_id=to_side,
            device_id_type=MESH,
        )

    for step in range(zs):
        for way in range(2):
            core_copy(way, step).start()
    for step in range(zs):
        for sub in range(subs):
            for way in range(2):
                if sub == 0:
                    core_copy(way, step).wait_recv()
                piece = at(owner(way, step), way, core)
                span = pl.ds(sub * step_rows, step_rows)
                value = part_ref[piece, span, :].astype(jnp.float32) + core_ref[way, step, span, :].astype(jnp.float32)
                if step > 0:
                    ring_copy(way, step - 1, sub).wait_recv()
                    value = value + ring_ref[way, step - 1, sub].astype(jnp.float32)
                stage_ref[way, step, sub] = value.astype(stage_ref.dtype)
                if step < zs - 1:
                    ring_copy(way, step, sub).start()
        if step == zs - 1:
            for sub in range(subs):
                side_copy(sub).start()
    share = 1.0 / (4 * zs)
    for sub in range(subs):
        side_copy(sub).wait_recv()
        span = pl.ds(sub * step_rows, step_rows)
        total = stage_ref[xlo, zs - 1, sub].astype(jnp.float32) + side_ref[sub].astype(jnp.float32)
        out_ref[span, :] = total * share
    for step in range(zs):
        for way in range(2):
            core_copy(way, step).wait_send()
            for sub in range(subs):
                if step < zs - 1:
                    ring_copy(way, step, sub).wait_send()
    for sub in range(subs):
        side_copy(sub).wait_send()


def reduce_rows(part, dp_count, collective_id, subs=2):
    zs = dp_count // 4
    width = part.shape[1]
    rows = part.shape[0] // dp_count
    kind = part.dtype
    return pl.pallas_call(
        functools.partial(reduce_kernel, zs, subs),
        out_shape=jax.ShapeDtypeStruct((rows, width), jnp.float32),
        in_specs=[pl.BlockSpec(memory_space=pltpu.VMEM)],
        out_specs=pl.BlockSpec(memory_space=pltpu.VMEM),
        scratch_shapes=[
            pltpu.VMEM((2, zs, rows, width), kind),
            pltpu.VMEM((2, zs - 1, subs, rows // subs, width), kind),
            pltpu.VMEM((2, zs, subs, rows // subs, width), kind),
            pltpu.VMEM((subs, rows // subs, width), kind),
            pltpu.SemaphoreType.DMA((2, zs)),
            pltpu.SemaphoreType.DMA((2, zs)),
            pltpu.SemaphoreType.DMA((2, zs - 1, subs)),
            pltpu.SemaphoreType.DMA((2, zs - 1, subs)),
            pltpu.SemaphoreType.DMA((subs,)),
            pltpu.SemaphoreType.DMA((subs,)),
        ],
        compiler_params=pltpu.CompilerParams(
            collective_id=collective_id, has_side_effects=True, vmem_limit_bytes=32 * 1024 * 1024
        ),
        cost_estimate=pl.CostEstimate(flops=40_000_000_000, bytes_accessed=7_000_000, transcendentals=0),
        name="reduce_rows",
    )(part.reshape(dp_count, rows, width))


def dispatch_masks(route_ids, experts, capacity):
    tokens = route_ids.shape[0]
    flat_ids = route_ids.reshape(-1)
    slot_total = flat_ids.shape[0]
    onehot = flat_ids[:, None] == jnp.arange(experts, dtype=jnp.int32)[None, :]
    order = jnp.arange(slot_total, dtype=jnp.int32)
    before = (order[:, None] > order[None, :]).astype(jnp.bfloat16)
    earlier = jnp.dot(before, onehot.astype(jnp.bfloat16), preferred_element_type=jnp.float32)
    ranking = jnp.sum(jnp.where(onehot, earlier, 0.0), axis=1).astype(jnp.int32)
    destination = (flat_ids * capacity + ranking).reshape(tokens, 2)
    rows = jnp.arange(experts * capacity, dtype=jnp.int32)
    first = rows[:, None] == destination[:, 0][None, :]
    second = rows[:, None] == destination[:, 1][None, :]
    return first, second


def dequantize(stash_rows, scale_rows):
    row_total = stash_rows.shape[0]
    blocks = scale_rows.shape[1]
    scaled = (
        stash_rows.reshape(row_total, blocks, -1).astype(jnp.float32)
        * scale_rows.astype(jnp.float32)[:, :, None]
    )
    return scaled.reshape(row_total, -1).astype(jnp.bfloat16)


def gated_backward(gate_up, back_hidden):
    hidden = back_hidden.shape[1]
    gate_value = gate_up[:, :hidden]
    up_value = gate_up[:, hidden:]
    sigmoid_gate = jax.nn.sigmoid(gate_value)
    grad_gate = back_hidden * up_value * sigmoid_gate * (1.0 + gate_value * (1.0 - sigmoid_gate))
    grad_up = back_hidden * gate_value * sigmoid_gate
    return jnp.concatenate([grad_gate, grad_up], axis=1).astype(jnp.bfloat16)


def exchange(rows, experts, capacity):
    width = rows.shape[1]
    moved = lax.all_to_all(
        rows.reshape(experts, capacity, width), ROW_AXES, split_axis=0, concat_axis=0, tiled=True
    )
    return moved.reshape(experts * capacity, width)


def plane_weights(w_down):
    planes = lax.axis_size("xlo")
    experts = lax.axis_size(ROW_AXES)
    copies = jnp.broadcast_to(w_down[None], (planes * experts,) + w_down.shape)
    mine = lax.all_to_all(copies, ("xlo",) + ROW_AXES, split_axis=0, concat_axis=0, tiled=True)
    return mine.reshape((planes, experts) + w_down.shape)


def relay_kernel(zs, grad_ref, ids_ref, gate_ref, weight_ref, out_ref,
                 slice_ref, wide_ref, pick_ref, stage_ref, back_ref,
                 own_sem, slice_send, slice_recv, weight_sem, weight_send, weight_recv, back_send, back_recv):
    z, xlo, core = ring_place()
    tokens = out_ref.shape[1]
    depth = slice_ref.shape[2]
    experts = weight_ref.shape[1]
    rows = weight_ref.shape[2]
    half = zs // 2
    offsets = []
    for d in range(1, half):
        offsets += [-d, d]
    offsets += [half, 0]
    twin = place(z, xlo, 1 - core)

    def peer(offset):
        return lax.rem(z + offset + zs, zs)

    def mirror(slot):
        return slot if slot >= zs - 2 else slot ^ 1

    greet([place(peer(offset), xlo, core) for offset in offsets[:-1]] + [twin])

    def columns(offset):
        return pl.ds(pl.multiple_of(peer(offset) * depth, depth), depth)

    def slice_copy(slot):
        return pltpu.make_async_remote_copy(
            src_ref=grad_ref.at[:, columns(offsets[slot])],
            dst_ref=slice_ref.at[mirror(slot)],
            send_sem=slice_send.at[slot],
            recv_sem=slice_recv.at[mirror(slot)],
            device_id=place(peer(offsets[slot]), xlo, core),
            device_id_type=MESH,
        )

    def back_copy(slot):
        return pltpu.make_async_remote_copy(
            src_ref=stage_ref.at[slot],
            dst_ref=back_ref.at[mirror(slot)],
            send_sem=back_send.at[slot],
            recv_sem=back_recv.at[mirror(slot)],
            device_id=place(peer(offsets[slot]), xlo, core),
            device_id_type=MESH,
        )

    def slice_arrival(slot):
        return pltpu.make_async_remote_copy(
            src_ref=slice_ref.at[slot],
            dst_ref=slice_ref.at[slot],
            send_sem=slice_send.at[slot],
            recv_sem=slice_recv.at[slot],
            device_id=twin,
            device_id_type=MESH,
        )

    def back_arrival(slot):
        return pltpu.make_async_remote_copy(
            src_ref=back_ref.at[slot],
            dst_ref=back_ref.at[slot],
            send_sem=back_send.at[slot],
            recv_sem=back_recv.at[slot],
            device_id=twin,
            device_id_type=MESH,
        )

    def weight_rows(plane, side):
        return wide_ref.at[:, pl.ds(pl.multiple_of((2 * plane + side) * rows, rows), rows), :]

    def weight_copy(plane):
        return pltpu.make_async_remote_copy(
            src_ref=weight_ref.at[plane],
            dst_ref=weight_rows(plane, core),
            send_sem=weight_send.at[plane],
            recv_sem=weight_recv.at[plane],
            device_id=twin,
            device_id_type=MESH,
        )

    def weight_arrival(plane):
        return pltpu.make_async_remote_copy(
            src_ref=weight_ref.at[plane],
            dst_ref=weight_rows(plane, 1 - core),
            send_sem=weight_send.at[plane],
            recv_sem=weight_recv.at[plane],
            device_id=twin,
            device_id_type=MESH,
        )

    keeps = [pltpu.make_async_copy(grad_ref.at[:, columns(0)], slice_ref.at[zs - 1], own_sem)]
    for plane in range(2):
        keeps.append(pltpu.make_async_copy(weight_ref.at[plane], weight_rows(plane, core), weight_sem.at[plane]))
    for slot in range(zs - 1):
        slice_copy(slot).start()
    for plane in range(2):
        weight_copy(plane).start()
    for keep in keeps:
        keep.start()
    for keep in keeps:
        keep.wait()
    for plane in range(2):
        weight_arrival(plane).wait_recv()
    for pair in range(half):
        for side in range(2):
            slot = 2 * pair + side
            if slot < zs - 1:
                slice_arrival(slot).wait_recv()
        pick_ref[...] = jnp.zeros_like(pick_ref)

        def per_expert(e, carry):
            wide = wide_ref[e]
            for side in range(2):
                slot = 2 * pair + side
                dense = jnp.dot(slice_ref[slot], wide, preferred_element_type=jnp.float32)
                first_row = pl.multiple_of(peer(offsets[slot]) * tokens, tokens)
                for k in range(2):
                    chosen = ids_ref[pl.ds(first_row, tokens), k : k + 1] == e
                    pick_ref[side, k] = jnp.where(chosen, dense, pick_ref[side, k])
            return carry

        lax.fori_loop(0, experts, per_expert, 0)
        for side in range(2):
            slot = 2 * pair + side
            stage_ref[slot] = pick_ref[side].astype(stage_ref.dtype)
            if slot < zs - 1:
                back_copy(slot).start()
    total = stage_ref[zs - 1].astype(jnp.float32)
    for slot in range(zs - 1):
        back_arrival(slot).wait_recv()
        total = total + back_ref[slot].astype(jnp.float32)
    for k in range(2):
        out_ref[k] = (total[k] * gate_ref[:, k : k + 1]).astype(out_ref.dtype)
    for slot in range(zs - 1):
        slice_copy(slot).wait_send()
        back_copy(slot).wait_send()
    for plane in range(2):
        weight_copy(plane).wait_send()


def hidden_gradient(out_grad, all_ids, gates, weights, zs):
    tokens, feature_width = out_grad.shape
    planes, experts, rows, hidden = weights.shape
    depth = feature_width // zs
    kind = out_grad.dtype
    vmem = pl.BlockSpec(memory_space=pltpu.VMEM)
    return pl.pallas_call(
        functools.partial(relay_kernel, zs),
        out_shape=jax.ShapeDtypeStruct((2, tokens, hidden), kind),
        in_specs=[pl.BlockSpec(memory_space=pl.ANY), vmem, vmem, pl.BlockSpec(memory_space=pl.ANY)],
        out_specs=vmem,
        scratch_shapes=[
            pltpu.VMEM((zs, tokens, depth), kind),
            pltpu.VMEM((experts, 2 * planes * rows, hidden), kind),
            pltpu.VMEM((2, 2, tokens, hidden), jnp.float32),
            pltpu.VMEM((zs, 2, tokens, hidden), kind),
            pltpu.VMEM((zs - 1, 2, tokens, hidden), kind),
            pltpu.SemaphoreType.DMA,
            pltpu.SemaphoreType.DMA((zs - 1,)),
            pltpu.SemaphoreType.DMA((zs - 1,)),
            pltpu.SemaphoreType.DMA((2,)),
            pltpu.SemaphoreType.DMA((2,)),
            pltpu.SemaphoreType.DMA((2,)),
            pltpu.SemaphoreType.DMA((zs - 1,)),
            pltpu.SemaphoreType.DMA((zs - 1,)),
        ],
        compiler_params=pltpu.CompilerParams(
            collective_id=1, has_side_effects=True, vmem_limit_bytes=24 * 1024 * 1024
        ),
        cost_estimate=pl.CostEstimate(flops=40_000_000_000, bytes_accessed=7_000_000, transcendentals=0),
        name="relay_hidden",
    )(out_grad, all_ids, gates, weights)


def on_device(stash, scales, out_grad, route_ids, gates, w_gate_up, w_down):
    tokens, feature_width = stash.shape
    hidden = w_down.shape[2]
    experts = lax.axis_size(ROW_AXES)
    dp_count = lax.axis_size(COLUMN_AXES)
    capacity = min(tokens, 7 * tokens // (2 * experts))
    first, second = dispatch_masks(route_ids, experts, capacity)
    picks = (first | second).astype(jnp.bfloat16)
    slots = jnp.concatenate([first, second], axis=1).astype(jnp.bfloat16)
    sent_x = jnp.dot(picks, dequantize(stash, scales), preferred_element_type=jnp.float32).astype(jnp.bfloat16)
    weight_in = w_gate_up[0]
    features = exchange(sent_x, experts, capacity)
    zs = lax.axis_size("z")
    all_ids = lax.all_gather(route_ids, "z", axis=0, tiled=True)
    weights = plane_weights(w_down[0])
    slot_hidden = hidden_gradient(out_grad, all_ids, gates, weights, zs).reshape(2 * tokens, hidden)
    sent_hidden = jnp.dot(slots, slot_hidden, preferred_element_type=jnp.float32).astype(jnp.bfloat16)
    back_hidden = exchange(sent_hidden, experts, capacity).astype(jnp.float32)
    gate_up = jnp.dot(features, weight_in, preferred_element_type=jnp.float32)
    hidden_grad = gated_backward(gate_up, back_hidden)
    slot_grads = lax.dot_general(
        hidden_grad, weight_in, (((1,), (1,)), ((), ())), preferred_element_type=jnp.float32
    ).astype(jnp.bfloat16)
    returned = exchange(slot_grads, experts, capacity)
    input_grad = lax.dot_general(
        picks, returned, (((0,), (0,)), ((), ())), preferred_element_type=jnp.float32
    ).astype(jnp.bfloat16)
    local_rows = feature_width // dp_count
    partial_grad = lax.dot_general(
        features, hidden_grad, (((0,), (0,)), ((), ())), preferred_element_type=jnp.float32
    ).astype(jnp.bfloat16)
    grad_gate_up = reduce_rows(partial_grad, dp_count, 2).reshape(1, local_rows, 2 * hidden)
    return (input_grad, grad_gate_up)


def solution(mesh):
    dp_count, experts = mesh.devices.shape
    split = Mesh(
        mesh.devices.reshape(dp_count // 4, 2, 2, 2, experts // 2), COLUMN_AXES + ROW_AXES
    )
    tokens = P(COLUMN_AXES + ROW_AXES, None)
    placed = (tokens, tokens, tokens, tokens, tokens, P(ROW_AXES, None, None), P(ROW_AXES, COLUMN_AXES, None))
    return jax.shard_map(
        on_device,
        mesh=split,
        in_specs=placed,
        out_specs=(tokens, P(ROW_AXES, COLUMN_AXES, None)),
        check_vma=False,
    )
```

```python
import functools

import jax
import jax.numpy as jnp
from jax import lax
from jax.experimental import pallas as pl
from jax.experimental.pallas import tpu as pltpu
from jax.sharding import Mesh
from jax.sharding import PartitionSpec as P

MESH = pl.DeviceIdType.MESH
COLUMN_AXES = ("z", "xlo", "core")
ROW_AXES = ("xhi", "y")


def ring_place():
    return lax.axis_index("z"), lax.axis_index("xlo"), lax.axis_index("core")


def place(z, xlo, core):
    return {"z": z, "xlo": xlo, "core": core}


def greet(partners):
    barrier = pltpu.get_barrier_semaphore()
    for partner in partners:
        pl.semaphore_signal(barrier, inc=1, device_id=partner, device_id_type=MESH)
    pl.semaphore_wait(barrier, len(partners))


def reduce_kernel(zs, subs, part_ref, out_ref, core_ref, ring_ref, stage_ref, side_ref,
                  core_send, core_recv, ring_send, ring_recv, side_send, side_recv):
    z, xlo, core = ring_place()
    rows = part_ref.shape[1]
    step_rows = rows // subs

    def at(zz, xx, cc):
        return zz * 4 + xx * 2 + cc

    up, down = lax.rem(z + 1, zs), lax.rem(z + zs - 1, zs)
    to_up, to_down = place(up, xlo, core), place(down, xlo, core)
    to_side, to_twin = place(z, 1 - xlo, core), place(z, xlo, 1 - core)
    greet((to_up, to_down, to_side, to_twin))

    def owner(way, step):
        return lax.rem(z + 2 * zs - 1 - step, zs) if way == 0 else lax.rem(z + 1 + step, zs)

    def core_copy(way, step):
        piece = owner(way, step)
        return pltpu.make_async_remote_copy(
            src_ref=part_ref.at[at(piece, way, 1 - core)],
            dst_ref=core_ref.at[way, step],
            send_sem=core_send.at[way, step],
            recv_sem=core_recv.at[way, step],
            device_id=to_twin,
            device_id_type=MESH,
        )

    def ring_copy(way, step, sub):
        return pltpu.make_async_remote_copy(
            src_ref=stage_ref.at[way, step, sub],
            dst_ref=ring_ref.at[way, step, sub],
            send_sem=ring_send.at[way, step, sub],
            recv_sem=ring_recv.at[way, step, sub],
            device_id=to_up if way == 0 else to_down,
            device_id_type=MESH,
        )

    def side_copy(sub):
        return pltpu.make_async_remote_copy(
            src_ref=stage_ref.at[1 - xlo, zs - 1, sub],
            dst_ref=side_ref.at[sub],
            send_sem=side_send.at[sub],
            recv_sem=side_recv.at[sub],
            device_id=to_side,
            device_id_type=MESH,
        )

    for step in range(zs):
        for way in range(2):
            core_copy(way, step).start()
    for step in range(zs):
        for sub in range(subs):
            for way in range(2):
                if sub == 0:
                    core_copy(way, step).wait_recv()
                piece = at(owner(way, step), way, core)
                span = pl.ds(sub * step_rows, step_rows)
                value = part_ref[piece, span, :].astype(jnp.float32) + core_ref[way, step, span, :].astype(jnp.float32)
                if step > 0:
                    ring_copy(way, step - 1, sub).wait_recv()
                    value = value + ring_ref[way, step - 1, sub].astype(jnp.float32)
                stage_ref[way, step, sub] = value.astype(stage_ref.dtype)
                if step < zs - 1:
                    ring_copy(way, step, sub).start()
        if step == zs - 1:
            for sub in range(subs):
                side_copy(sub).start()
    share = 1.0 / (4 * zs)
    for sub in range(subs):
        side_copy(sub).wait_recv()
        span = pl.ds(sub * step_rows, step_rows)
        total = stage_ref[xlo, zs - 1, sub].astype(jnp.float32) + side_ref[sub].astype(jnp.float32)
        out_ref[span, :] = total * share
    for step in range(zs):
        for way in range(2):
            core_copy(way, step).wait_send()
            for sub in range(subs):
                if step < zs - 1:
                    ring_copy(way, step, sub).wait_send()
    for sub in range(subs):
        side_copy(sub).wait_send()


def reduce_rows(part, dp_count, collective_id, subs=2):
    zs = dp_count // 4
    width = part.shape[1]
    rows = part.shape[0] // dp_count
    kind = part.dtype
    return pl.pallas_call(
        functools.partial(reduce_kernel, zs, subs),
        out_shape=jax.ShapeDtypeStruct((rows, width), jnp.float32),
        in_specs=[pl.BlockSpec(memory_space=pltpu.VMEM)],
        out_specs=pl.BlockSpec(memory_space=pltpu.VMEM),
        scratch_shapes=[
            pltpu.VMEM((2, zs, rows, width), kind),
            pltpu.VMEM((2, zs - 1, subs, rows // subs, width), kind),
            pltpu.VMEM((2, zs, subs, rows // subs, width), kind),
            pltpu.VMEM((subs, rows // subs, width), kind),
            pltpu.SemaphoreType.DMA((2, zs)),
            pltpu.SemaphoreType.DMA((2, zs)),
            pltpu.SemaphoreType.DMA((2, zs - 1, subs)),
            pltpu.SemaphoreType.DMA((2, zs - 1, subs)),
            pltpu.SemaphoreType.DMA((subs,)),
            pltpu.SemaphoreType.DMA((subs,)),
        ],
        compiler_params=pltpu.CompilerParams(
            collective_id=collective_id, has_side_effects=True, vmem_limit_bytes=32 * 1024 * 1024
        ),
        cost_estimate=pl.CostEstimate(flops=40_000_000_000, bytes_accessed=7_000_000, transcendentals=0),
        name="reduce_rows",
    )(part.reshape(dp_count, rows, width))


def dispatch_masks(route_ids, experts, capacity, stride):
    tokens = route_ids.shape[0]
    flat_ids = route_ids.reshape(-1)
    slot_total = flat_ids.shape[0]
    onehot = flat_ids[:, None] == jnp.arange(experts, dtype=jnp.int32)[None, :]
    order = jnp.arange(slot_total, dtype=jnp.int32)
    before = (order[:, None] > order[None, :]).astype(jnp.bfloat16)
    earlier = jnp.dot(before, onehot.astype(jnp.bfloat16), preferred_element_type=jnp.float32)
    ranking = jnp.sum(jnp.where(onehot, earlier, 0.0), axis=1).astype(jnp.int32)

    def match(pitch):
        target = (flat_ids * pitch + ranking).reshape(tokens, 2)
        rows = jnp.arange(experts * pitch, dtype=jnp.int32)[:, None]
        return rows == target[:, 0][None, :], rows == target[:, 1][None, :]

    first, second = match(capacity)
    slots = jnp.concatenate(match(stride), axis=1).astype(jnp.bfloat16)
    return (first | second).astype(jnp.bfloat16), slots


def dequantize(stash_rows, scale_rows):
    row_total = stash_rows.shape[0]
    blocks = scale_rows.shape[1]
    scaled = (
        stash_rows.reshape(row_total, blocks, -1).astype(jnp.float32)
        * scale_rows.astype(jnp.float32)[:, :, None]
    )
    return scaled.reshape(row_total, -1).astype(jnp.bfloat16)


def gated_backward(gate_up, back_hidden):
    hidden = back_hidden.shape[1]
    gate_value = gate_up[:, :hidden]
    up_value = gate_up[:, hidden:]
    sigmoid_gate = jax.nn.sigmoid(gate_value)
    grad_gate = back_hidden * up_value * sigmoid_gate * (1.0 + gate_value * (1.0 - sigmoid_gate))
    grad_up = back_hidden * gate_value * sigmoid_gate
    return jnp.concatenate([grad_gate, grad_up], axis=1).astype(jnp.bfloat16)


def exchange(rows, experts, capacity):
    width = rows.shape[1]
    moved = lax.all_to_all(
        rows.reshape(experts, capacity, width), ROW_AXES, split_axis=0, concat_axis=0, tiled=True
    )
    return moved.reshape(experts * capacity, width)


def plane_weights(w_down):
    planes = lax.axis_size("xlo")
    experts = lax.axis_size(ROW_AXES)
    copies = jnp.broadcast_to(w_down[None], (planes * experts,) + w_down.shape)
    mine = lax.all_to_all(copies, ("xlo",) + ROW_AXES, split_axis=0, concat_axis=0, tiled=True)
    return mine.reshape((planes, experts) + w_down.shape)


def relay_kernel(zs, sent_ref, grad_ref, ids_in_ref, gate_ref, weight_ref, slots_ref, rows_ref, out_ref,
                 pass_ref, rows_send, rows_recv, pass_sem, ids_ref, ids_send, ids_recv,
                 tail_ref, tail_send, tail_recv, tail_sem, slice_ref, wide_ref, pick_ref, stage_ref, back_ref,
                 own_sem, slice_send, slice_recv, weight_sem, weight_send, weight_recv, back_send, back_recv):
    z, xlo, core = ring_place()
    tokens = slice_ref.shape[1]
    depth = slice_ref.shape[2]
    experts_out = sent_ref.shape[0]
    mine = lax.axis_index("xhi") * (experts_out // 2) + lax.axis_index("y")

    def row_of(shift):
        return lax.rem(mine + shift, experts_out)

    def row_place(shift):
        row = row_of(shift)
        return {"xhi": row // (experts_out // 2), "y": lax.rem(row, experts_out // 2)}

    experts = weight_ref.shape[1]
    rows = weight_ref.shape[2]
    half = zs // 2
    offsets = []
    for d in range(1, half):
        offsets += [-d, d]
    offsets += [half, 0]
    twin = place(z, xlo, 1 - core)

    def peer(offset):
        return lax.rem(z + offset + zs, zs)

    def mirror(slot):
        return slot if slot >= zs - 2 else slot ^ 1

    greet(
        [place(peer(offset), xlo, core) for offset in offsets[:-1]]
        + [twin]
        + [row_place(shift) for shift in range(1, experts_out)]
    )

    def rows_copy(shift):
        return pltpu.make_async_remote_copy(
            src_ref=sent_ref.at[row_of(shift)],
            dst_ref=rows_ref.at[mine],
            send_sem=rows_send.at[shift - 1],
            recv_sem=rows_recv.at[shift - 1],
            device_id=row_place(shift),
            device_id_type=MESH,
        )

    def rows_arrival(shift):
        source = row_of(experts_out - shift)
        return pltpu.make_async_remote_copy(
            src_ref=sent_ref.at[source],
            dst_ref=rows_ref.at[source],
            send_sem=rows_send.at[shift - 1],
            recv_sem=rows_recv.at[shift - 1],
            device_id=twin,
            device_id_type=MESH,
        )

    def tail_copy(shift):
        return pltpu.make_async_remote_copy(
            src_ref=tail_ref.at[row_of(shift)],
            dst_ref=out_ref.at[mine],
            send_sem=tail_send.at[shift - 1],
            recv_sem=tail_recv.at[shift - 1],
            device_id=row_place(shift),
            device_id_type=MESH,
        )

    def tail_arrival(shift):
        source = row_of(experts_out - shift)
        return pltpu.make_async_remote_copy(
            src_ref=tail_ref.at[source],
            dst_ref=out_ref.at[source],
            send_sem=tail_send.at[shift - 1],
            recv_sem=tail_recv.at[shift - 1],
            device_id=twin,
            device_id_type=MESH,
        )

    def ids_copy(slot):
        return pltpu.make_async_remote_copy(
            src_ref=ids_in_ref,
            dst_ref=ids_ref.at[mirror(slot)],
            send_sem=ids_send.at[slot],
            recv_sem=ids_recv.at[mirror(slot)],
            device_id=place(peer(offsets[slot]), xlo, core),
            device_id_type=MESH,
        )

    def ids_arrival(slot):
        return pltpu.make_async_remote_copy(
            src_ref=ids_ref.at[slot],
            dst_ref=ids_ref.at[slot],
            send_sem=ids_send.at[slot],
            recv_sem=ids_recv.at[slot],
            device_id=twin,
            device_id_type=MESH,
        )

    def columns(offset):
        return pl.ds(pl.multiple_of(peer(offset) * depth, depth), depth)

    def slice_copy(slot):
        return pltpu.make_async_remote_copy(
            src_ref=grad_ref.at[:, columns(offsets[slot])],
            dst_ref=slice_ref.at[mirror(slot)],
            send_sem=slice_send.at[slot],
            recv_sem=slice_recv.at[mirror(slot)],
            device_id=place(peer(offsets[slot]), xlo, core),
            device_id_type=MESH,
        )

    def back_copy(slot):
        return pltpu.make_async_remote_copy(
            src_ref=stage_ref.at[slot],
            dst_ref=back_ref.at[mirror(slot)],
            send_sem=back_send.at[slot],
            recv_sem=back_recv.at[mirror(slot)],
            device_id=place(peer(offsets[slot]), xlo, core),
            device_id_type=MESH,
        )

    def slice_arrival(slot):
        return pltpu.make_async_remote_copy(
            src_ref=slice_ref.at[slot],
            dst_ref=slice_ref.at[slot],
            send_sem=slice_send.at[slot],
            recv_sem=slice_recv.at[slot],
            device_id=twin,
            device_id_type=MESH,
        )

    def back_arrival(slot):
        return pltpu.make_async_remote_copy(
            src_ref=back_ref.at[slot],
            dst_ref=back_ref.at[slot],
            send_sem=back_send.at[slot],
            recv_sem=back_recv.at[slot],
            device_id=twin,
            device_id_type=MESH,
        )

    def weight_rows(plane, side):
        return wide_ref.at[:, pl.ds(pl.multiple_of((2 * plane + side) * rows, rows), rows), :]

    def weight_copy(plane):
        return pltpu.make_async_remote_copy(
            src_ref=weight_ref.at[plane],
            dst_ref=weight_rows(plane, core),
            send_sem=weight_send.at[plane],
            recv_sem=weight_recv.at[plane],
            device_id=twin,
            device_id_type=MESH,
        )

    def weight_arrival(plane):
        return pltpu.make_async_remote_copy(
            src_ref=weight_ref.at[plane],
            dst_ref=weight_rows(plane, 1 - core),
            send_sem=weight_send.at[plane],
            recv_sem=weight_recv.at[plane],
            device_id=twin,
            device_id_type=MESH,
        )

    keeps = [pltpu.make_async_copy(grad_ref.at[:, columns(0)], slice_ref.at[zs - 1], own_sem)]
    for plane in range(2):
        keeps.append(pltpu.make_async_copy(weight_ref.at[plane], weight_rows(plane, core), weight_sem.at[plane]))
    for shift in range(1, experts_out):
        rows_copy(shift).start()
    for slot in range(zs - 1):
        ids_copy(slot).start()
    for slot in range(zs - 1):
        slice_copy(slot).start()
    for plane in range(2):
        weight_copy(plane).start()
    pass_in = pltpu.make_async_copy(sent_ref.at[mine], pass_ref, pass_sem)
    pass_out = pltpu.make_async_copy(pass_ref, rows_ref.at[mine], pass_sem)
    pass_in.start()
    ids_ref[zs - 1] = ids_in_ref[...]
    for keep in keeps:
        keep.start()
    for keep in keeps:
        keep.wait()
    pass_in.wait()
    pass_out.start()
    for plane in range(2):
        weight_arrival(plane).wait_recv()
    for pair in range(half):
        for side in range(2):
            slot = 2 * pair + side
            if slot < zs - 1:
                ids_arrival(slot).wait_recv()
                slice_arrival(slot).wait_recv()
        pick_ref[...] = jnp.zeros_like(pick_ref)

        def per_expert(e, carry):
            wide = wide_ref[e]
            for side in range(2):
                slot = 2 * pair + side
                dense = jnp.dot(slice_ref[slot], wide, preferred_element_type=jnp.float32)
                for k in range(2):
                    chosen = ids_ref[slot, :, k : k + 1] == e
                    pick_ref[side, k] = jnp.where(chosen, dense, pick_ref[side, k])
            return carry

        lax.fori_loop(0, experts, per_expert, 0)
        for side in range(2):
            slot = 2 * pair + side
            stage_ref[slot] = pick_ref[side].astype(stage_ref.dtype)
            if slot < zs - 1:
                back_copy(slot).start()
    total = stage_ref[zs - 1].astype(jnp.float32)
    for slot in range(zs - 1):
        back_arrival(slot).wait_recv()
        total = total + back_ref[slot].astype(jnp.float32)
    weighted = [(total[k] * gate_ref[:, k : k + 1]).astype(tail_ref.dtype) for k in range(2)]
    placed = jnp.dot(slots_ref[...], jnp.concatenate(weighted, axis=0), preferred_element_type=jnp.float32)
    tail_ref[...] = placed.astype(tail_ref.dtype).reshape(tail_ref.shape)
    for shift in range(1, experts_out):
        tail_copy(shift).start()
    keep_tail = pltpu.make_async_copy(tail_ref.at[mine], out_ref.at[mine], tail_sem)
    keep_tail.start()
    for shift in range(1, experts_out):
        rows_arrival(shift).wait_recv()
    for slot in range(zs - 1):
        ids_copy(slot).wait_send()
        slice_copy(slot).wait_send()
        back_copy(slot).wait_send()
    for plane in range(2):
        weight_copy(plane).wait_send()
    pass_out.wait()
    for shift in range(1, experts_out):
        tail_arrival(shift).wait_recv()
        rows_copy(shift).wait_send()
        tail_copy(shift).wait_send()
    keep_tail.wait()


def relay(sent_x, out_grad, route_ids, gates, weights, slots, zs):
    tokens, feature_width = out_grad.shape
    planes, experts, rows, hidden = weights.shape
    depth = feature_width // zs
    tail_rows = slots.shape[0] // experts
    kind = out_grad.dtype
    vmem = pl.BlockSpec(memory_space=pltpu.VMEM)
    anywhere = pl.BlockSpec(memory_space=pl.ANY)
    pairs = pltpu.SemaphoreType.DMA((zs - 1,))
    others = pltpu.SemaphoreType.DMA((experts - 1,))
    return pl.pallas_call(
        functools.partial(relay_kernel, zs),
        out_shape=(
            jax.ShapeDtypeStruct(sent_x.shape, kind),
            jax.ShapeDtypeStruct((experts, tail_rows, hidden), kind),
        ),
        in_specs=[anywhere, anywhere, vmem, vmem, anywhere, vmem],
        out_specs=(anywhere, anywhere),
        scratch_shapes=[
            pltpu.VMEM(sent_x.shape[1:], kind),
            others,
            others,
            pltpu.SemaphoreType.DMA,
            pltpu.VMEM((zs,) + route_ids.shape, route_ids.dtype),
            pairs,
            pairs,
            pltpu.VMEM((experts, tail_rows, hidden), kind),
            others,
            others,
            pltpu.SemaphoreType.DMA,
            pltpu.VMEM((zs, tokens, depth), kind),
            pltpu.VMEM((experts, 2 * planes * rows, hidden), kind),
            pltpu.VMEM((2, 2, tokens, hidden), jnp.float32),
            pltpu.VMEM((zs, 2, tokens, hidden), kind),
            pltpu.VMEM((zs - 1, 2, tokens, hidden), kind),
            pltpu.SemaphoreType.DMA,
            pairs,
            pairs,
            pltpu.SemaphoreType.DMA((2,)),
            pltpu.SemaphoreType.DMA((2,)),
            pltpu.SemaphoreType.DMA((2,)),
            pairs,
            pairs,
        ],
        compiler_params=pltpu.CompilerParams(
            collective_id=1, has_side_effects=True, vmem_limit_bytes=24 * 1024 * 1024
        ),
        cost_estimate=pl.CostEstimate(flops=40_000_000_000, bytes_accessed=7_000_000, transcendentals=0),
        name="relay",
    )(sent_x, out_grad, route_ids, gates, weights, slots)


def on_device(stash, scales, out_grad, route_ids, gates, w_gate_up, w_down):
    tokens, feature_width = stash.shape
    hidden = w_down.shape[2]
    experts = lax.axis_size(ROW_AXES)
    dp_count = lax.axis_size(COLUMN_AXES)
    capacity = min(tokens, 7 * tokens // (2 * experts))
    stride = -(-capacity // 16) * 16
    picks, slots = dispatch_masks(route_ids, experts, capacity, stride)
    sent_x = jnp.dot(picks, dequantize(stash, scales), preferred_element_type=jnp.float32).astype(jnp.bfloat16)
    weight_in = w_gate_up[0]
    zs = lax.axis_size("z")
    weights = plane_weights(w_down[0])
    got_x, got_hidden = relay(
        sent_x.reshape(experts, capacity, feature_width), out_grad, route_ids, gates, weights, slots, zs
    )
    features = got_x.reshape(experts * capacity, feature_width)
    back_hidden = got_hidden[:, :capacity].reshape(experts * capacity, hidden).astype(jnp.float32)
    gate_up = jnp.dot(features, weight_in, preferred_element_type=jnp.float32)
    hidden_grad = gated_backward(gate_up, back_hidden)
    slot_grads = lax.dot_general(
        hidden_grad, weight_in, (((1,), (1,)), ((), ())), preferred_element_type=jnp.float32
    ).astype(jnp.bfloat16)
    returned = exchange(slot_grads, experts, capacity)
    input_grad = lax.dot_general(
        picks, returned, (((0,), (0,)), ((), ())), preferred_element_type=jnp.float32
    ).astype(jnp.bfloat16)
    local_rows = feature_width // dp_count
    partial_grad = lax.dot_general(
        features, hidden_grad, (((0,), (0,)), ((), ())), preferred_element_type=jnp.float32
    ).astype(jnp.bfloat16)
    grad_gate_up = reduce_rows(partial_grad, dp_count, 2).reshape(1, local_rows, 2 * hidden)
    return (input_grad, grad_gate_up)


def solution(mesh):
    dp_count, experts = mesh.devices.shape
    split = Mesh(
        mesh.devices.reshape(dp_count // 4, 2, 2, 2, experts // 2), COLUMN_AXES + ROW_AXES
    )
    tokens = P(COLUMN_AXES + ROW_AXES, None)
    placed = (tokens, tokens, tokens, tokens, tokens, P(ROW_AXES, None, None), P(ROW_AXES, COLUMN_AXES, None))
    return jax.shard_map(
        on_device,
        mesh=split,
        in_specs=placed,
        out_specs=(tokens, P(ROW_AXES, COLUMN_AXES, None)),
        check_vma=False,
    )
```

```python
import functools

import jax
import jax.numpy as jnp
from jax import lax
from jax.experimental import pallas as pl
from jax.experimental.pallas import tpu as pltpu
from jax.sharding import Mesh
from jax.sharding import PartitionSpec as P

MESH = pl.DeviceIdType.MESH
COLUMN_AXES = ("z", "xlo", "core")
ROW_AXES = ("xhi", "y")


def ring_place():
    return lax.axis_index("z"), lax.axis_index("xlo"), lax.axis_index("core")


def place(z, xlo, core):
    return {"z": z, "xlo": xlo, "core": core}


def greet(partners):
    barrier = pltpu.get_barrier_semaphore()
    for partner in partners:
        pl.semaphore_signal(barrier, inc=1, device_id=partner, device_id_type=MESH)
    pl.semaphore_wait(barrier, len(partners))


def reduce_kernel(zs, subs, part_ref, out_ref, core_ref, ring_ref, stage_ref, side_ref,
                  core_send, core_recv, ring_send, ring_recv, side_send, side_recv):
    z, xlo, core = ring_place()
    rows = part_ref.shape[1]
    step_rows = rows // subs

    def at(zz, xx, cc):
        return zz * 4 + xx * 2 + cc

    up, down = lax.rem(z + 1, zs), lax.rem(z + zs - 1, zs)
    to_up, to_down = place(up, xlo, core), place(down, xlo, core)
    to_side, to_twin = place(z, 1 - xlo, core), place(z, xlo, 1 - core)
    greet((to_up, to_down, to_side, to_twin))

    def owner(way, step):
        return lax.rem(z + 2 * zs - 1 - step, zs) if way == 0 else lax.rem(z + 1 + step, zs)

    def core_copy(way, step):
        piece = owner(way, step)
        return pltpu.make_async_remote_copy(
            src_ref=part_ref.at[at(piece, way, 1 - core)],
            dst_ref=core_ref.at[way, step],
            send_sem=core_send.at[way, step],
            recv_sem=core_recv.at[way, step],
            device_id=to_twin,
            device_id_type=MESH,
        )

    def ring_copy(way, step, sub):
        return pltpu.make_async_remote_copy(
            src_ref=stage_ref.at[way, step, sub],
            dst_ref=ring_ref.at[way, step, sub],
            send_sem=ring_send.at[way, step, sub],
            recv_sem=ring_recv.at[way, step, sub],
            device_id=to_up if way == 0 else to_down,
            device_id_type=MESH,
        )

    def side_copy(sub):
        return pltpu.make_async_remote_copy(
            src_ref=stage_ref.at[1 - xlo, zs - 1, sub],
            dst_ref=side_ref.at[sub],
            send_sem=side_send.at[sub],
            recv_sem=side_recv.at[sub],
            device_id=to_side,
            device_id_type=MESH,
        )

    for step in range(zs):
        for way in range(2):
            core_copy(way, step).start()
    for step in range(zs):
        for sub in range(subs):
            for way in range(2):
                if sub == 0:
                    core_copy(way, step).wait_recv()
                piece = at(owner(way, step), way, core)
                span = pl.ds(sub * step_rows, step_rows)
                value = part_ref[piece, span, :].astype(jnp.float32) + core_ref[way, step, span, :].astype(jnp.float32)
                if step > 0:
                    ring_copy(way, step - 1, sub).wait_recv()
                    value = value + ring_ref[way, step - 1, sub].astype(jnp.float32)
                stage_ref[way, step, sub] = value.astype(stage_ref.dtype)
                if step < zs - 1:
                    ring_copy(way, step, sub).start()
        if step == zs - 1:
            for sub in range(subs):
                side_copy(sub).start()
    share = 1.0 / (4 * zs)
    for sub in range(subs):
        side_copy(sub).wait_recv()
        span = pl.ds(sub * step_rows, step_rows)
        total = stage_ref[xlo, zs - 1, sub].astype(jnp.float32) + side_ref[sub].astype(jnp.float32)
        out_ref[span, :] = total * share
    for step in range(zs):
        for way in range(2):
            core_copy(way, step).wait_send()
            for sub in range(subs):
                if step < zs - 1:
                    ring_copy(way, step, sub).wait_send()
    for sub in range(subs):
        side_copy(sub).wait_send()


def reduce_rows(part, dp_count, collective_id, subs=2):
    zs = dp_count // 4
    width = part.shape[1]
    rows = part.shape[0] // dp_count
    kind = part.dtype
    return pl.pallas_call(
        functools.partial(reduce_kernel, zs, subs),
        out_shape=jax.ShapeDtypeStruct((rows, width), jnp.float32),
        in_specs=[pl.BlockSpec(memory_space=pltpu.VMEM)],
        out_specs=pl.BlockSpec(memory_space=pltpu.VMEM),
        scratch_shapes=[
            pltpu.VMEM((2, zs, rows, width), kind),
            pltpu.VMEM((2, zs - 1, subs, rows // subs, width), kind),
            pltpu.VMEM((2, zs, subs, rows // subs, width), kind),
            pltpu.VMEM((subs, rows // subs, width), kind),
            pltpu.SemaphoreType.DMA((2, zs)),
            pltpu.SemaphoreType.DMA((2, zs)),
            pltpu.SemaphoreType.DMA((2, zs - 1, subs)),
            pltpu.SemaphoreType.DMA((2, zs - 1, subs)),
            pltpu.SemaphoreType.DMA((subs,)),
            pltpu.SemaphoreType.DMA((subs,)),
        ],
        compiler_params=pltpu.CompilerParams(
            collective_id=collective_id, has_side_effects=True, vmem_limit_bytes=32 * 1024 * 1024
        ),
        cost_estimate=pl.CostEstimate(flops=40_000_000_000, bytes_accessed=7_000_000, transcendentals=0),
        name="reduce_rows",
    )(part.reshape(dp_count, rows, width))


def dispatch_masks(route_ids, experts, capacity, stride):
    tokens = route_ids.shape[0]
    flat_ids = route_ids.reshape(-1)
    slot_total = flat_ids.shape[0]
    onehot = flat_ids[:, None] == jnp.arange(experts, dtype=jnp.int32)[None, :]
    order = jnp.arange(slot_total, dtype=jnp.int32)
    before = (order[:, None] > order[None, :]).astype(jnp.bfloat16)
    earlier = jnp.dot(before, onehot.astype(jnp.bfloat16), preferred_element_type=jnp.float32)
    ranking = jnp.sum(jnp.where(onehot, earlier, 0.0), axis=1).astype(jnp.int32)

    def match(pitch):
        target = (flat_ids * pitch + ranking).reshape(tokens, 2)
        rows = jnp.arange(experts * pitch, dtype=jnp.int32)[:, None]
        return rows == target[:, 0][None, :], rows == target[:, 1][None, :]

    first, second = match(capacity)
    slots = jnp.concatenate(match(stride), axis=1).astype(jnp.bfloat16)
    return (first | second).astype(jnp.bfloat16), slots


def dequantize(stash_rows, scale_rows):
    row_total = stash_rows.shape[0]
    blocks = scale_rows.shape[1]
    scaled = (
        stash_rows.reshape(row_total, blocks, -1).astype(jnp.float32)
        * scale_rows.astype(jnp.float32)[:, :, None]
    )
    return scaled.reshape(row_total, -1).astype(jnp.bfloat16)


def gated_backward(gate_up, back_hidden):
    hidden = back_hidden.shape[1]
    gate_value = gate_up[:, :hidden]
    up_value = gate_up[:, hidden:]
    sigmoid_gate = jax.nn.sigmoid(gate_value)
    grad_gate = back_hidden * up_value * sigmoid_gate * (1.0 + gate_value * (1.0 - sigmoid_gate))
    grad_up = back_hidden * gate_value * sigmoid_gate
    return jnp.concatenate([grad_gate, grad_up], axis=1).astype(jnp.bfloat16)


def exchange(rows, experts, capacity):
    width = rows.shape[1]
    moved = lax.all_to_all(
        rows.reshape(experts, capacity, width), ROW_AXES, split_axis=0, concat_axis=0, tiled=True
    )
    return moved.reshape(experts * capacity, width)


def plane_weights(w_down):
    planes = lax.axis_size("xlo")
    experts = lax.axis_size(ROW_AXES)
    copies = jnp.broadcast_to(w_down[None], (planes * experts,) + w_down.shape)
    mine = lax.all_to_all(copies, ("xlo",) + ROW_AXES, split_axis=0, concat_axis=0, tiled=True)
    return mine.reshape((planes, experts) + w_down.shape)


def relay_kernel(zs, grad_ref, ids_in_ref, gate_ref, weight_ref, slots_ref, out_ref, ids_ref, ids_send, ids_recv,
                 tail_ref, tail_send, tail_recv, tail_sem, slice_ref, wide_ref, pick_ref, stage_ref, back_ref,
                 own_sem, slice_send, slice_recv, weight_sem, weight_send, weight_recv, back_send, back_recv):
    z, xlo, core = ring_place()
    tokens = slice_ref.shape[1]
    depth = slice_ref.shape[2]
    experts_out = out_ref.shape[0]
    mine = lax.axis_index("xhi") * (experts_out // 2) + lax.axis_index("y")

    def row_of(shift):
        return lax.rem(mine + shift, experts_out)

    def row_place(shift):
        row = row_of(shift)
        return {"xhi": row // (experts_out // 2), "y": lax.rem(row, experts_out // 2)}

    experts = weight_ref.shape[1]
    rows = weight_ref.shape[2]
    half = zs // 2
    offsets = []
    for d in range(1, half):
        offsets += [-d, d]
    offsets += [half, 0]
    twin = place(z, xlo, 1 - core)

    def peer(offset):
        return lax.rem(z + offset + zs, zs)

    def mirror(slot):
        return slot if slot >= zs - 2 else slot ^ 1

    greet(
        [place(peer(offset), xlo, core) for offset in offsets[:-1]]
        + [twin]
        + [row_place(shift) for shift in range(1, experts_out)]
    )

    def tail_copy(shift):
        return pltpu.make_async_remote_copy(
            src_ref=tail_ref.at[row_of(shift)],
            dst_ref=out_ref.at[mine],
            send_sem=tail_send.at[shift - 1],
            recv_sem=tail_recv.at[shift - 1],
            device_id=row_place(shift),
            device_id_type=MESH,
        )

    def tail_arrival(shift):
        source = row_of(experts_out - shift)
        return pltpu.make_async_remote_copy(
            src_ref=tail_ref.at[source],
            dst_ref=out_ref.at[source],
            send_sem=tail_send.at[shift - 1],
            recv_sem=tail_recv.at[shift - 1],
            device_id=twin,
            device_id_type=MESH,
        )

    def ids_copy(slot):
        return pltpu.make_async_remote_copy(
            src_ref=ids_in_ref,
            dst_ref=ids_ref.at[mirror(slot)],
            send_sem=ids_send.at[slot],
            recv_sem=ids_recv.at[mirror(slot)],
            device_id=place(peer(offsets[slot]), xlo, core),
            device_id_type=MESH,
        )

    def ids_arrival(slot):
        return pltpu.make_async_remote_copy(
            src_ref=ids_ref.at[slot],
            dst_ref=ids_ref.at[slot],
            send_sem=ids_send.at[slot],
            recv_sem=ids_recv.at[slot],
            device_id=twin,
            device_id_type=MESH,
        )

    def columns(offset):
        return pl.ds(pl.multiple_of(peer(offset) * depth, depth), depth)

    def slice_copy(slot):
        return pltpu.make_async_remote_copy(
            src_ref=grad_ref.at[:, columns(offsets[slot])],
            dst_ref=slice_ref.at[mirror(slot)],
            send_sem=slice_send.at[slot],
            recv_sem=slice_recv.at[mirror(slot)],
            device_id=place(peer(offsets[slot]), xlo, core),
            device_id_type=MESH,
        )

    def back_copy(slot):
        return pltpu.make_async_remote_copy(
            src_ref=stage_ref.at[slot],
            dst_ref=back_ref.at[mirror(slot)],
            send_sem=back_send.at[slot],
            recv_sem=back_recv.at[mirror(slot)],
            device_id=place(peer(offsets[slot]), xlo, core),
            device_id_type=MESH,
        )

    def slice_arrival(slot):
        return pltpu.make_async_remote_copy(
            src_ref=slice_ref.at[slot],
            dst_ref=slice_ref.at[slot],
            send_sem=slice_send.at[slot],
            recv_sem=slice_recv.at[slot],
            device_id=twin,
            device_id_type=MESH,
        )

    def back_arrival(slot):
        return pltpu.make_async_remote_copy(
            src_ref=back_ref.at[slot],
            dst_ref=back_ref.at[slot],
            send_sem=back_send.at[slot],
            recv_sem=back_recv.at[slot],
            device_id=twin,
            device_id_type=MESH,
        )

    def weight_rows(plane, side):
        return wide_ref.at[:, pl.ds(pl.multiple_of((2 * plane + side) * rows, rows), rows), :]

    def weight_copy(plane):
        return pltpu.make_async_remote_copy(
            src_ref=weight_ref.at[plane],
            dst_ref=weight_rows(plane, core),
            send_sem=weight_send.at[plane],
            recv_sem=weight_recv.at[plane],
            device_id=twin,
            device_id_type=MESH,
        )

    def weight_arrival(plane):
        return pltpu.make_async_remote_copy(
            src_ref=weight_ref.at[plane],
            dst_ref=weight_rows(plane, 1 - core),
            send_sem=weight_send.at[plane],
            recv_sem=weight_recv.at[plane],
            device_id=twin,
            device_id_type=MESH,
        )

    keeps = [pltpu.make_async_copy(grad_ref.at[:, columns(0)], slice_ref.at[zs - 1], own_sem)]
    for plane in range(2):
        keeps.append(pltpu.make_async_copy(weight_ref.at[plane], weight_rows(plane, core), weight_sem.at[plane]))
    for slot in range(zs - 1):
        ids_copy(slot).start()
    for slot in range(zs - 1):
        slice_copy(slot).start()
    for plane in range(2):
        weight_copy(plane).start()
    ids_ref[zs - 1] = ids_in_ref[...]
    for keep in keeps:
        keep.start()
    for keep in keeps:
        keep.wait()
    for plane in range(2):
        weight_arrival(plane).wait_recv()
    for pair in range(half):
        for side in range(2):
            slot = 2 * pair + side
            if slot < zs - 1:
                ids_arrival(slot).wait_recv()
                slice_arrival(slot).wait_recv()
        pick_ref[...] = jnp.zeros_like(pick_ref)

        def per_expert(e, carry):
            wide = wide_ref[e]
            for side in range(2):
                slot = 2 * pair + side
                dense = jnp.dot(slice_ref[slot], wide, preferred_element_type=jnp.float32)
                for k in range(2):
                    chosen = ids_ref[slot, :, k : k + 1] == e
                    pick_ref[side, k] = jnp.where(chosen, dense, pick_ref[side, k])
            return carry

        lax.fori_loop(0, experts, per_expert, 0)
        for side in range(2):
            slot = 2 * pair + side
            stage_ref[slot] = pick_ref[side].astype(stage_ref.dtype)
            if slot < zs - 1:
                back_copy(slot).start()
    total = stage_ref[zs - 1].astype(jnp.float32)
    for slot in range(zs - 1):
        back_arrival(slot).wait_recv()
        total = total + back_ref[slot].astype(jnp.float32)
    weighted = [(total[k] * gate_ref[:, k : k + 1]).astype(tail_ref.dtype) for k in range(2)]
    placed = jnp.dot(slots_ref[...], jnp.concatenate(weighted, axis=0), preferred_element_type=jnp.float32)
    tail_ref[...] = placed.astype(tail_ref.dtype).reshape(tail_ref.shape)
    for shift in range(1, experts_out):
        tail_copy(shift).start()
    keep_tail = pltpu.make_async_copy(tail_ref.at[mine], out_ref.at[mine], tail_sem)
    keep_tail.start()
    for slot in range(zs - 1):
        ids_copy(slot).wait_send()
        slice_copy(slot).wait_send()
        back_copy(slot).wait_send()
    for plane in range(2):
        weight_copy(plane).wait_send()
    for shift in range(1, experts_out):
        tail_arrival(shift).wait_recv()
        tail_copy(shift).wait_send()
    keep_tail.wait()


def relay(out_grad, route_ids, gates, weights, slots, zs):
    tokens, feature_width = out_grad.shape
    planes, experts, rows, hidden = weights.shape
    depth = feature_width // zs
    tail_rows = slots.shape[0] // experts
    kind = out_grad.dtype
    vmem = pl.BlockSpec(memory_space=pltpu.VMEM)
    anywhere = pl.BlockSpec(memory_space=pl.ANY)
    pairs = pltpu.SemaphoreType.DMA((zs - 1,))
    others = pltpu.SemaphoreType.DMA((experts - 1,))
    return pl.pallas_call(
        functools.partial(relay_kernel, zs),
        out_shape=jax.ShapeDtypeStruct((experts, tail_rows, hidden), kind),
        in_specs=[anywhere, vmem, vmem, anywhere, vmem],
        out_specs=anywhere,
        scratch_shapes=[
            pltpu.VMEM((zs,) + route_ids.shape, route_ids.dtype),
            pairs,
            pairs,
            pltpu.VMEM((experts, tail_rows, hidden), kind),
            others,
            others,
            pltpu.SemaphoreType.DMA,
            pltpu.VMEM((zs, tokens, depth), kind),
            pltpu.VMEM((experts, 2 * planes * rows, hidden), kind),
            pltpu.VMEM((2, 2, tokens, hidden), jnp.float32),
            pltpu.VMEM((zs, 2, tokens, hidden), kind),
            pltpu.VMEM((zs - 1, 2, tokens, hidden), kind),
            pltpu.SemaphoreType.DMA,
            pairs,
            pairs,
            pltpu.SemaphoreType.DMA((2,)),
            pltpu.SemaphoreType.DMA((2,)),
            pltpu.SemaphoreType.DMA((2,)),
            pairs,
            pairs,
        ],
        compiler_params=pltpu.CompilerParams(
            collective_id=1, has_side_effects=True, vmem_limit_bytes=24 * 1024 * 1024
        ),
        cost_estimate=pl.CostEstimate(flops=40_000_000_000, bytes_accessed=7_000_000, transcendentals=0),
        name="relay",
    )(out_grad, route_ids, gates, weights, slots)


def on_device(stash, scales, out_grad, route_ids, gates, w_gate_up, w_down):
    tokens, feature_width = stash.shape
    hidden = w_down.shape[2]
    experts = lax.axis_size(ROW_AXES)
    dp_count = lax.axis_size(COLUMN_AXES)
    capacity = min(tokens, 7 * tokens // (2 * experts))
    stride = -(-capacity // 16) * 16
    picks, slots = dispatch_masks(route_ids, experts, capacity, stride)
    sent_x = jnp.dot(picks, dequantize(stash, scales), preferred_element_type=jnp.float32).astype(jnp.bfloat16)
    weight_in = w_gate_up[0]
    zs = lax.axis_size("z")
    weights = plane_weights(w_down[0])
    features = exchange(sent_x, experts, capacity)
    got_hidden = relay(out_grad, route_ids, gates, weights, slots, zs)
    back_hidden = got_hidden[:, :capacity].reshape(experts * capacity, hidden).astype(jnp.float32)
    gate_up = jnp.dot(features, weight_in, preferred_element_type=jnp.float32)
    hidden_grad = gated_backward(gate_up, back_hidden)
    slot_grads = lax.dot_general(
        hidden_grad, weight_in, (((1,), (1,)), ((), ())), preferred_element_type=jnp.float32
    ).astype(jnp.bfloat16)
    returned = exchange(slot_grads, experts, capacity)
    input_grad = lax.dot_general(
        picks, returned, (((0,), (0,)), ((), ())), preferred_element_type=jnp.float32
    ).astype(jnp.bfloat16)
    local_rows = feature_width // dp_count
    partial_grad = lax.dot_general(
        features, hidden_grad, (((0,), (0,)), ((), ())), preferred_element_type=jnp.float32
    ).astype(jnp.bfloat16)
    grad_gate_up = reduce_rows(partial_grad, dp_count, 2).reshape(1, local_rows, 2 * hidden)
    return (input_grad, grad_gate_up)


def solution(mesh):
    dp_count, experts = mesh.devices.shape
    split = Mesh(
        mesh.devices.reshape(dp_count // 4, 2, 2, 2, experts // 2), COLUMN_AXES + ROW_AXES
    )
    tokens = P(COLUMN_AXES + ROW_AXES, None)
    placed = (tokens, tokens, tokens, tokens, tokens, P(ROW_AXES, None, None), P(ROW_AXES, COLUMN_AXES, None))
    return jax.shard_map(
        on_device,
        mesh=split,
        in_specs=placed,
        out_specs=(tokens, P(ROW_AXES, COLUMN_AXES, None)),
        check_vma=False,
    )
```

```python
import functools

import jax
import jax.numpy as jnp
from jax import lax
from jax.experimental import pallas as pl
from jax.experimental.pallas import tpu as pltpu
from jax.sharding import Mesh
from jax.sharding import PartitionSpec as P

MESH = pl.DeviceIdType.MESH
COLUMN_AXES = ("z", "xlo", "core")
ROW_AXES = ("xhi", "y")


def ring_place():
    return lax.axis_index("z"), lax.axis_index("xlo"), lax.axis_index("core")


def place(z, xlo, core):
    return {"z": z, "xlo": xlo, "core": core}


def greet(partners):
    barrier = pltpu.get_barrier_semaphore()
    for partner in partners:
        pl.semaphore_signal(barrier, inc=1, device_id=partner, device_id_type=MESH)
    pl.semaphore_wait(barrier, len(partners))


def reduce_kernel(zs, subs, part_ref, out_ref, core_ref, ring_ref, stage_ref, side_ref,
                  core_send, core_recv, ring_send, ring_recv, side_send, side_recv):
    z, xlo, core = ring_place()
    rows = part_ref.shape[1]
    step_rows = rows // subs

    def at(zz, xx, cc):
        return zz * 4 + xx * 2 + cc

    up, down = lax.rem(z + 1, zs), lax.rem(z + zs - 1, zs)
    to_up, to_down = place(up, xlo, core), place(down, xlo, core)
    to_side, to_twin = place(z, 1 - xlo, core), place(z, xlo, 1 - core)
    greet((to_up, to_down, to_side, to_twin))

    def owner(way, step):
        return lax.rem(z + 2 * zs - 1 - step, zs) if way == 0 else lax.rem(z + 1 + step, zs)

    def core_copy(way, step):
        piece = owner(way, step)
        return pltpu.make_async_remote_copy(
            src_ref=part_ref.at[at(piece, way, 1 - core)],
            dst_ref=core_ref.at[way, step],
            send_sem=core_send.at[way, step],
            recv_sem=core_recv.at[way, step],
            device_id=to_twin,
            device_id_type=MESH,
        )

    def ring_copy(way, step, sub):
        return pltpu.make_async_remote_copy(
            src_ref=stage_ref.at[way, step, sub],
            dst_ref=ring_ref.at[way, step, sub],
            send_sem=ring_send.at[way, step, sub],
            recv_sem=ring_recv.at[way, step, sub],
            device_id=to_up if way == 0 else to_down,
            device_id_type=MESH,
        )

    def side_copy(sub):
        return pltpu.make_async_remote_copy(
            src_ref=stage_ref.at[1 - xlo, zs - 1, sub],
            dst_ref=side_ref.at[sub],
            send_sem=side_send.at[sub],
            recv_sem=side_recv.at[sub],
            device_id=to_side,
            device_id_type=MESH,
        )

    for step in range(zs):
        for way in range(2):
            core_copy(way, step).start()
    for step in range(zs):
        for sub in range(subs):
            for way in range(2):
                if sub == 0:
                    core_copy(way, step).wait_recv()
                piece = at(owner(way, step), way, core)
                span = pl.ds(sub * step_rows, step_rows)
                value = part_ref[piece, span, :].astype(jnp.float32) + core_ref[way, step, span, :].astype(jnp.float32)
                if step > 0:
                    ring_copy(way, step - 1, sub).wait_recv()
                    value = value + ring_ref[way, step - 1, sub].astype(jnp.float32)
                stage_ref[way, step, sub] = value.astype(stage_ref.dtype)
                if step < zs - 1:
                    ring_copy(way, step, sub).start()
        if step == zs - 1:
            for sub in range(subs):
                side_copy(sub).start()
    share = 1.0 / (4 * zs)
    for sub in range(subs):
        side_copy(sub).wait_recv()
        span = pl.ds(sub * step_rows, step_rows)
        total = stage_ref[xlo, zs - 1, sub].astype(jnp.float32) + side_ref[sub].astype(jnp.float32)
        out_ref[span, :] = total * share
    for step in range(zs):
        for way in range(2):
            core_copy(way, step).wait_send()
            for sub in range(subs):
                if step < zs - 1:
                    ring_copy(way, step, sub).wait_send()
    for sub in range(subs):
        side_copy(sub).wait_send()


def reduce_rows(part, dp_count, collective_id, subs=2):
    zs = dp_count // 4
    width = part.shape[1]
    rows = part.shape[0] // dp_count
    kind = part.dtype
    return pl.pallas_call(
        functools.partial(reduce_kernel, zs, subs),
        out_shape=jax.ShapeDtypeStruct((rows, width), jnp.float32),
        in_specs=[pl.BlockSpec(memory_space=pltpu.VMEM)],
        out_specs=pl.BlockSpec(memory_space=pltpu.VMEM),
        scratch_shapes=[
            pltpu.VMEM((2, zs, rows, width), kind),
            pltpu.VMEM((2, zs - 1, subs, rows // subs, width), kind),
            pltpu.VMEM((2, zs, subs, rows // subs, width), kind),
            pltpu.VMEM((subs, rows // subs, width), kind),
            pltpu.SemaphoreType.DMA((2, zs)),
            pltpu.SemaphoreType.DMA((2, zs)),
            pltpu.SemaphoreType.DMA((2, zs - 1, subs)),
            pltpu.SemaphoreType.DMA((2, zs - 1, subs)),
            pltpu.SemaphoreType.DMA((subs,)),
            pltpu.SemaphoreType.DMA((subs,)),
        ],
        compiler_params=pltpu.CompilerParams(
            collective_id=collective_id, has_side_effects=True, vmem_limit_bytes=32 * 1024 * 1024
        ),
        cost_estimate=pl.CostEstimate(flops=40_000_000_000, bytes_accessed=7_000_000, transcendentals=0),
        name="reduce_rows",
    )(part.reshape(dp_count, rows, width))


def dispatch_masks(route_ids, experts, capacity, stride):
    tokens = route_ids.shape[0]
    flat_ids = route_ids.reshape(-1)
    slot_total = flat_ids.shape[0]
    onehot = flat_ids[:, None] == jnp.arange(experts, dtype=jnp.int32)[None, :]
    order = jnp.arange(slot_total, dtype=jnp.int32)
    before = (order[:, None] > order[None, :]).astype(jnp.bfloat16)
    earlier = jnp.dot(before, onehot.astype(jnp.bfloat16), preferred_element_type=jnp.float32)
    ranking = jnp.sum(jnp.where(onehot, earlier, 0.0), axis=1).astype(jnp.int32)

    def match(pitch):
        target = (flat_ids * pitch + ranking).reshape(tokens, 2)
        rows = jnp.arange(experts * pitch, dtype=jnp.int32)[:, None]
        return rows == target[:, 0][None, :], rows == target[:, 1][None, :]

    first, second = match(capacity)
    slots = jnp.concatenate(match(stride), axis=1).astype(jnp.bfloat16)
    return (first | second).astype(jnp.bfloat16), slots


def dequantize(stash_rows, scale_rows):
    row_total = stash_rows.shape[0]
    blocks = scale_rows.shape[1]
    scaled = (
        stash_rows.reshape(row_total, blocks, -1).astype(jnp.float32)
        * scale_rows.astype(jnp.float32)[:, :, None]
    )
    return scaled.reshape(row_total, -1).astype(jnp.bfloat16)


def gated_backward(gate_up, back_hidden):
    hidden = back_hidden.shape[1]
    gate_value = gate_up[:, :hidden]
    up_value = gate_up[:, hidden:]
    sigmoid_gate = jax.nn.sigmoid(gate_value)
    grad_gate = back_hidden * up_value * sigmoid_gate * (1.0 + gate_value * (1.0 - sigmoid_gate))
    grad_up = back_hidden * gate_value * sigmoid_gate
    return jnp.concatenate([grad_gate, grad_up], axis=1).astype(jnp.bfloat16)


def exchange(rows, experts, capacity):
    width = rows.shape[1]
    moved = lax.all_to_all(
        rows.reshape(experts, capacity, width), ROW_AXES, split_axis=0, concat_axis=0, tiled=True
    )
    return moved.reshape(experts * capacity, width)


def plane_weights(w_down):
    planes = lax.axis_size("xlo")
    experts = lax.axis_size(ROW_AXES)
    copies = jnp.broadcast_to(w_down[None], (planes * experts,) + w_down.shape)
    mine = lax.all_to_all(copies, ("xlo",) + ROW_AXES, split_axis=0, concat_axis=0, tiled=True)
    return mine.reshape((planes, experts) + w_down.shape)


def relay_kernel(zs, grad_ref, ids_in_ref, gate_ref, weight_ref, slots_ref, out_ref, ids_ref, turn_ref, ids_send, ids_recv,
                 tail_ref, tail_send, tail_recv, tail_sem, slice_ref, wide_ref, pick_ref, stage_ref, back_ref,
                 own_sem, slice_send, slice_recv, weight_sem, weight_send, weight_recv, back_send, back_recv):
    z, xlo, core = ring_place()
    tokens = slice_ref.shape[1]
    depth = slice_ref.shape[2]
    experts_out = out_ref.shape[0]
    mine = lax.axis_index("xhi") * (experts_out // 2) + lax.axis_index("y")

    def row_of(shift):
        return lax.rem(mine + shift, experts_out)

    def row_place(shift):
        row = row_of(shift)
        return {"xhi": row // (experts_out // 2), "y": lax.rem(row, experts_out // 2)}

    experts = weight_ref.shape[1]
    rows = weight_ref.shape[2]
    half = zs // 2
    offsets = []
    for d in range(1, half):
        offsets += [-d, d]
    offsets += [half, 0]
    twin = place(z, xlo, 1 - core)

    def peer(offset):
        return lax.rem(z + offset + zs, zs)

    def mirror(slot):
        return slot if slot >= zs - 2 else slot ^ 1

    greet(
        [place(peer(offset), xlo, core) for offset in offsets[:-1]]
        + [twin]
        + [row_place(shift) for shift in range(1, experts_out)]
    )

    def tail_copy(shift):
        return pltpu.make_async_remote_copy(
            src_ref=tail_ref.at[row_of(shift)],
            dst_ref=out_ref.at[mine],
            send_sem=tail_send.at[shift - 1],
            recv_sem=tail_recv.at[shift - 1],
            device_id=row_place(shift),
            device_id_type=MESH,
        )

    def tail_arrival(shift):
        source = row_of(experts_out - shift)
        return pltpu.make_async_remote_copy(
            src_ref=tail_ref.at[source],
            dst_ref=out_ref.at[source],
            send_sem=tail_send.at[shift - 1],
            recv_sem=tail_recv.at[shift - 1],
            device_id=twin,
            device_id_type=MESH,
        )

    def ids_copy(slot):
        return pltpu.make_async_remote_copy(
            src_ref=ids_in_ref,
            dst_ref=ids_ref.at[mirror(slot)],
            send_sem=ids_send.at[slot],
            recv_sem=ids_recv.at[mirror(slot)],
            device_id=place(peer(offsets[slot]), xlo, core),
            device_id_type=MESH,
        )

    def ids_arrival(slot):
        return pltpu.make_async_remote_copy(
            src_ref=ids_ref.at[slot],
            dst_ref=ids_ref.at[slot],
            send_sem=ids_send.at[slot],
            recv_sem=ids_recv.at[slot],
            device_id=twin,
            device_id_type=MESH,
        )

    def columns(offset):
        return pl.ds(pl.multiple_of(peer(offset) * depth, depth), depth)

    def slice_copy(slot):
        return pltpu.make_async_remote_copy(
            src_ref=grad_ref.at[:, columns(offsets[slot])],
            dst_ref=slice_ref.at[mirror(slot)],
            send_sem=slice_send.at[slot],
            recv_sem=slice_recv.at[mirror(slot)],
            device_id=place(peer(offsets[slot]), xlo, core),
            device_id_type=MESH,
        )

    def back_copy(slot):
        return pltpu.make_async_remote_copy(
            src_ref=stage_ref.at[slot],
            dst_ref=back_ref.at[mirror(slot)],
            send_sem=back_send.at[slot],
            recv_sem=back_recv.at[mirror(slot)],
            device_id=place(peer(offsets[slot]), xlo, core),
            device_id_type=MESH,
        )

    def slice_arrival(slot):
        return pltpu.make_async_remote_copy(
            src_ref=slice_ref.at[slot],
            dst_ref=slice_ref.at[slot],
            send_sem=slice_send.at[slot],
            recv_sem=slice_recv.at[slot],
            device_id=twin,
            device_id_type=MESH,
        )

    def back_arrival(slot):
        return pltpu.make_async_remote_copy(
            src_ref=back_ref.at[slot],
            dst_ref=back_ref.at[slot],
            send_sem=back_send.at[slot],
            recv_sem=back_recv.at[slot],
            device_id=twin,
            device_id_type=MESH,
        )

    def weight_rows(plane, side):
        return wide_ref.at[:, pl.ds(pl.multiple_of((2 * plane + side) * rows, rows), rows), :]

    def weight_copy(plane):
        return pltpu.make_async_remote_copy(
            src_ref=weight_ref.at[plane],
            dst_ref=weight_rows(plane, core),
            send_sem=weight_send.at[plane],
            recv_sem=weight_recv.at[plane],
            device_id=twin,
            device_id_type=MESH,
        )

    def weight_arrival(plane):
        return pltpu.make_async_remote_copy(
            src_ref=weight_ref.at[plane],
            dst_ref=weight_rows(plane, 1 - core),
            send_sem=weight_send.at[plane],
            recv_sem=weight_recv.at[plane],
            device_id=twin,
            device_id_type=MESH,
        )

    keeps = [pltpu.make_async_copy(grad_ref.at[:, columns(0)], slice_ref.at[zs - 1], own_sem)]
    for plane in range(2):
        keeps.append(pltpu.make_async_copy(weight_ref.at[plane], weight_rows(plane, core), weight_sem.at[plane]))
    for slot in range(zs - 1):
        ids_copy(slot).start()
    for slot in range(zs - 1):
        slice_copy(slot).start()
    for plane in range(2):
        weight_copy(plane).start()
    ids_ref[zs - 1] = ids_in_ref[...]
    for keep in keeps:
        keep.start()
    for keep in keeps:
        keep.wait()
    for plane in range(2):
        weight_arrival(plane).wait_recv()
    for pair in range(half):
        for side in range(2):
            slot = 2 * pair + side
            if slot < zs - 1:
                ids_arrival(slot).wait_recv()
                slice_arrival(slot).wait_recv()
        pick_ref[...] = jnp.zeros_like(pick_ref)
        for side in range(2):
            tall = jnp.concatenate([ids_ref[2 * pair + side]] * (tokens // ids_ref.shape[1]), axis=0)
            turn_ref[pl.ds(side * tokens, tokens), :] = tall.T

        def per_expert(e, carry):
            both = slice_ref[pl.ds(2 * pair, 2)].reshape(2 * tokens, depth)
            dense = jnp.dot(both, wide_ref[e], preferred_element_type=jnp.float32)
            for k in range(2):
                pick_ref[k] = jnp.where(turn_ref[:, k : k + 1] == e, dense, pick_ref[k])
            return carry

        lax.fori_loop(0, experts, per_expert, 0)
        for side in range(2):
            slot = 2 * pair + side
            for k in range(2):
                stage_ref[slot, k] = pick_ref[k, pl.ds(side * tokens, tokens), :].astype(stage_ref.dtype)
            if slot < zs - 1:
                back_copy(slot).start()
    total = stage_ref[zs - 1].astype(jnp.float32)
    for slot in range(zs - 1):
        back_arrival(slot).wait_recv()
        total = total + back_ref[slot].astype(jnp.float32)
    weighted = [(total[k] * gate_ref[:, k : k + 1]).astype(tail_ref.dtype) for k in range(2)]
    placed = jnp.dot(slots_ref[...], jnp.concatenate(weighted, axis=0), preferred_element_type=jnp.float32)
    tail_ref[...] = placed.astype(tail_ref.dtype).reshape(tail_ref.shape)
    for shift in range(1, experts_out):
        tail_copy(shift).start()
    keep_tail = pltpu.make_async_copy(tail_ref.at[mine], out_ref.at[mine], tail_sem)
    keep_tail.start()
    for slot in range(zs - 1):
        ids_copy(slot).wait_send()
        slice_copy(slot).wait_send()
        back_copy(slot).wait_send()
    for plane in range(2):
        weight_copy(plane).wait_send()
    for shift in range(1, experts_out):
        tail_arrival(shift).wait_recv()
        tail_copy(shift).wait_send()
    keep_tail.wait()


def relay(out_grad, route_ids, gates, weights, slots, zs):
    tokens, feature_width = out_grad.shape
    planes, experts, rows, hidden = weights.shape
    depth = feature_width // zs
    tail_rows = slots.shape[0] // experts
    kind = out_grad.dtype
    vmem = pl.BlockSpec(memory_space=pltpu.VMEM)
    anywhere = pl.BlockSpec(memory_space=pl.ANY)
    pairs = pltpu.SemaphoreType.DMA((zs - 1,))
    others = pltpu.SemaphoreType.DMA((experts - 1,))
    return pl.pallas_call(
        functools.partial(relay_kernel, zs),
        out_shape=jax.ShapeDtypeStruct((experts, tail_rows, hidden), kind),
        in_specs=[anywhere, vmem, vmem, anywhere, vmem],
        out_specs=anywhere,
        scratch_shapes=[
            pltpu.VMEM((zs,) + route_ids.shape, route_ids.dtype),
            pltpu.VMEM((2 * tokens, tokens), route_ids.dtype),
            pairs,
            pairs,
            pltpu.VMEM((experts, tail_rows, hidden), kind),
            others,
            others,
            pltpu.SemaphoreType.DMA,
            pltpu.VMEM((zs, tokens, depth), kind),
            pltpu.VMEM((experts, 2 * planes * rows, hidden), kind),
            pltpu.VMEM((2, 2 * tokens, hidden), jnp.float32),
            pltpu.VMEM((zs, 2, tokens, hidden), kind),
            pltpu.VMEM((zs - 1, 2, tokens, hidden), kind),
            pltpu.SemaphoreType.DMA,
            pairs,
            pairs,
            pltpu.SemaphoreType.DMA((2,)),
            pltpu.SemaphoreType.DMA((2,)),
            pltpu.SemaphoreType.DMA((2,)),
            pairs,
            pairs,
        ],
        compiler_params=pltpu.CompilerParams(
            collective_id=1, has_side_effects=True, vmem_limit_bytes=24 * 1024 * 1024
        ),
        cost_estimate=pl.CostEstimate(flops=40_000_000_000, bytes_accessed=7_000_000, transcendentals=0),
        name="relay",
    )(out_grad, route_ids, gates, weights, slots)


def on_device(stash, scales, out_grad, route_ids, gates, w_gate_up, w_down):
    tokens, feature_width = stash.shape
    hidden = w_down.shape[2]
    experts = lax.axis_size(ROW_AXES)
    dp_count = lax.axis_size(COLUMN_AXES)
    capacity = min(tokens, 7 * tokens // (2 * experts))
    stride = -(-capacity // 16) * 16
    picks, slots = dispatch_masks(route_ids, experts, capacity, stride)
    sent_x = jnp.dot(picks, dequantize(stash, scales), preferred_element_type=jnp.float32).astype(jnp.bfloat16)
    weight_in = w_gate_up[0]
    zs = lax.axis_size("z")
    weights = plane_weights(w_down[0])
    features = exchange(sent_x, experts, capacity)
    id_rows = jnp.pad(route_ids.T, ((0, 6), (0, 0)))
    got_hidden = relay(out_grad, id_rows, gates, weights, slots, zs)
    back_hidden = got_hidden[:, :capacity].reshape(experts * capacity, hidden).astype(jnp.float32)
    gate_up = jnp.dot(features, weight_in, preferred_element_type=jnp.float32)
    hidden_grad = gated_backward(gate_up, back_hidden)
    slot_grads = lax.dot_general(
        hidden_grad, weight_in, (((1,), (1,)), ((), ())), preferred_element_type=jnp.float32
    ).astype(jnp.bfloat16)
    returned = exchange(slot_grads, experts, capacity)
    input_grad = lax.dot_general(
        picks, returned, (((0,), (0,)), ((), ())), preferred_element_type=jnp.float32
    ).astype(jnp.bfloat16)
    local_rows = feature_width // dp_count
    partial_grad = lax.dot_general(
        features, hidden_grad, (((0,), (0,)), ((), ())), preferred_element_type=jnp.float32
    ).astype(jnp.bfloat16)
    grad_gate_up = reduce_rows(partial_grad, dp_count, 2).reshape(1, local_rows, 2 * hidden)
    return (input_grad, grad_gate_up)


def solution(mesh):
    dp_count, experts = mesh.devices.shape
    split = Mesh(
        mesh.devices.reshape(dp_count // 4, 2, 2, 2, experts // 2), COLUMN_AXES + ROW_AXES
    )
    tokens = P(COLUMN_AXES + ROW_AXES, None)
    placed = (tokens, tokens, tokens, tokens, tokens, P(ROW_AXES, None, None), P(ROW_AXES, COLUMN_AXES, None))
    return jax.shard_map(
        on_device,
        mesh=split,
        in_specs=placed,
        out_specs=(tokens, P(ROW_AXES, COLUMN_AXES, None)),
        check_vma=False,
    )
```

```python
import functools

import jax
import jax.numpy as jnp
from jax import lax
from jax.experimental import pallas as pl
from jax.experimental.pallas import tpu as pltpu
from jax.sharding import Mesh
from jax.sharding import PartitionSpec as P

MESH = pl.DeviceIdType.MESH
COLUMN_AXES = ("z", "xlo", "core")
ROW_AXES = ("xhi", "y")


def ring_place():
    return lax.axis_index("z"), lax.axis_index("xlo"), lax.axis_index("core")


def place(z, xlo, core):
    return {"z": z, "xlo": xlo, "core": core}


def greet(partners):
    barrier = pltpu.get_barrier_semaphore()
    for partner in partners:
        pl.semaphore_signal(barrier, inc=1, device_id=partner, device_id_type=MESH)
    pl.semaphore_wait(barrier, len(partners))


def reduce_kernel(zs, subs, part_ref, out_ref, core_ref, ring_ref, stage_ref, side_ref,
                  core_send, core_recv, ring_send, ring_recv, side_send, side_recv):
    z, xlo, core = ring_place()
    rows = part_ref.shape[1]
    step_rows = rows // subs

    def at(zz, xx, cc):
        return zz * 4 + xx * 2 + cc

    up, down = lax.rem(z + 1, zs), lax.rem(z + zs - 1, zs)
    to_up, to_down = place(up, xlo, core), place(down, xlo, core)
    to_side, to_twin = place(z, 1 - xlo, core), place(z, xlo, 1 - core)
    greet((to_up, to_down, to_side, to_twin))

    def owner(way, step):
        return lax.rem(z + 2 * zs - 1 - step, zs) if way == 0 else lax.rem(z + 1 + step, zs)

    def core_copy(way, step):
        piece = owner(way, step)
        return pltpu.make_async_remote_copy(
            src_ref=part_ref.at[at(piece, way, 1 - core)],
            dst_ref=core_ref.at[way, step],
            send_sem=core_send.at[way, step],
            recv_sem=core_recv.at[way, step],
            device_id=to_twin,
            device_id_type=MESH,
        )

    def ring_copy(way, step, sub):
        return pltpu.make_async_remote_copy(
            src_ref=stage_ref.at[way, step, sub],
            dst_ref=ring_ref.at[way, step, sub],
            send_sem=ring_send.at[way, step, sub],
            recv_sem=ring_recv.at[way, step, sub],
            device_id=to_up if way == 0 else to_down,
            device_id_type=MESH,
        )

    def side_copy(sub):
        return pltpu.make_async_remote_copy(
            src_ref=stage_ref.at[1 - xlo, zs - 1, sub],
            dst_ref=side_ref.at[sub],
            send_sem=side_send.at[sub],
            recv_sem=side_recv.at[sub],
            device_id=to_side,
            device_id_type=MESH,
        )

    for step in range(zs):
        for way in range(2):
            core_copy(way, step).start()
    for step in range(zs):
        for sub in range(subs):
            for way in range(2):
                if sub == 0:
                    core_copy(way, step).wait_recv()
                piece = at(owner(way, step), way, core)
                span = pl.ds(sub * step_rows, step_rows)
                value = part_ref[piece, span, :].astype(jnp.float32) + core_ref[way, step, span, :].astype(jnp.float32)
                if step > 0:
                    ring_copy(way, step - 1, sub).wait_recv()
                    value = value + ring_ref[way, step - 1, sub].astype(jnp.float32)
                stage_ref[way, step, sub] = value.astype(stage_ref.dtype)
                if step < zs - 1:
                    ring_copy(way, step, sub).start()
        if step == zs - 1:
            for sub in range(subs):
                side_copy(sub).start()
    share = 1.0 / (4 * zs)
    for sub in range(subs):
        side_copy(sub).wait_recv()
        span = pl.ds(sub * step_rows, step_rows)
        total = stage_ref[xlo, zs - 1, sub].astype(jnp.float32) + side_ref[sub].astype(jnp.float32)
        out_ref[span, :] = total * share
    for step in range(zs):
        for way in range(2):
            core_copy(way, step).wait_send()
            for sub in range(subs):
                if step < zs - 1:
                    ring_copy(way, step, sub).wait_send()
    for sub in range(subs):
        side_copy(sub).wait_send()


def reduce_rows(part, dp_count, collective_id, subs=2):
    zs = dp_count // 4
    width = part.shape[1]
    rows = part.shape[0] // dp_count
    kind = part.dtype
    return pl.pallas_call(
        functools.partial(reduce_kernel, zs, subs),
        out_shape=jax.ShapeDtypeStruct((rows, width), jnp.float32),
        in_specs=[pl.BlockSpec(memory_space=pltpu.VMEM)],
        out_specs=pl.BlockSpec(memory_space=pltpu.VMEM),
        scratch_shapes=[
            pltpu.VMEM((2, zs, rows, width), kind),
            pltpu.VMEM((2, zs - 1, subs, rows // subs, width), kind),
            pltpu.VMEM((2, zs, subs, rows // subs, width), kind),
            pltpu.VMEM((subs, rows // subs, width), kind),
            pltpu.SemaphoreType.DMA((2, zs)),
            pltpu.SemaphoreType.DMA((2, zs)),
            pltpu.SemaphoreType.DMA((2, zs - 1, subs)),
            pltpu.SemaphoreType.DMA((2, zs - 1, subs)),
            pltpu.SemaphoreType.DMA((subs,)),
            pltpu.SemaphoreType.DMA((subs,)),
        ],
        compiler_params=pltpu.CompilerParams(
            collective_id=collective_id, has_side_effects=True, vmem_limit_bytes=32 * 1024 * 1024
        ),
        cost_estimate=pl.CostEstimate(flops=40_000_000_000, bytes_accessed=7_000_000, transcendentals=0),
        name="reduce_rows",
    )(part.reshape(dp_count, rows, width))


def gated_backward(gate_up, back_hidden):
    hidden = back_hidden.shape[1]
    gate_value = gate_up[:, :hidden]
    up_value = gate_up[:, hidden:]
    sigmoid_gate = jax.nn.sigmoid(gate_value)
    grad_gate = back_hidden * up_value * sigmoid_gate * (1.0 + gate_value * (1.0 - sigmoid_gate))
    grad_up = back_hidden * gate_value * sigmoid_gate
    return jnp.concatenate([grad_gate, grad_up], axis=1).astype(jnp.bfloat16)


def exchange(rows, experts, capacity):
    width = rows.shape[1]
    moved = lax.all_to_all(
        rows.reshape(experts, capacity, width), ROW_AXES, split_axis=0, concat_axis=0, tiled=True
    )
    return moved.reshape(experts * capacity, width)


def front_kernel(xs, ys, capacity, stride, pieces, ids_ref, stash_ref, scale_ref, weight_ref,
                 rows_ref, plane_ref, picks_ref, slots_ref,
                 build_ref, build_sem, keep_sem, y_send, y_recv, x_send, x_recv, yx_send, yx_recv, xy_send, xy_recv):
    xlo, xhi, y = lax.axis_index("xlo"), lax.axis_index("xhi"), lax.axis_index("y")
    x = xhi * 2 + xlo
    tokens, width = stash_ref.shape
    half = weight_ref.shape[0] // 2
    step = width // pieces

    def x_at(shift):
        return lax.rem(x + shift + xs, xs)

    def y_at(shift):
        return lax.rem(y + shift + ys, ys)

    def x_place(shift):
        return {"xlo": lax.rem(x_at(shift), 2), "xhi": x_at(shift) // 2}

    def y_place(shift):
        return {"y": y_at(shift)}

    def landed(xx, yy, part):
        return plane_ref.at[lax.rem(xx, 2), (xx // 2) * ys + yy, pl.ds(part * half, half), :]

    def moved(source, target, send, recv, device):
        return pltpu.make_async_remote_copy(
            src_ref=source, dst_ref=target, send_sem=send, recv_sem=recv, device_id=device, device_id_type=MESH
        )

    greet([x_place(k) for k in range(1, xs)] + [y_place(k) for k in range(1, ys)])
    own = [weight_ref.at[pl.ds(part * half, half), :] for part in range(2)]
    keep = pltpu.make_async_copy(weight_ref, plane_ref.at[xlo, xhi * ys + y], keep_sem)
    keep.start()
    sends, waits = [], []

    def send(copy):
        copy.start()
        sends.append(copy)

    for k in range(1, ys):
        send(moved(own[0], landed(x, y, 0), y_send.at[k - 1], y_recv.at[k - 1], y_place(k)))
    for k in range(1, xs):
        send(moved(own[1], landed(x, y, 1), x_send.at[k - 1], x_recv.at[k - 1], x_place(k)))
    for k in range(1, xs):
        send(moved(own[0], landed(x, y, 0), yx_send.at[0, k - 1], yx_recv.at[0, k - 1], x_place(k)))
    for k in range(1, ys):
        send(moved(own[1], landed(x, y, 1), xy_send.at[0, k - 1], xy_recv.at[0, k - 1], y_place(k)))

    expert = lax.broadcasted_iota(jnp.int32, ids_ref.shape, 0)
    first, second = ids_ref[0:1, :], ids_ref[1:2, :]
    named = jnp.where((expert == first) | (expert == second), 1.0, 0.0).astype(jnp.bfloat16)
    ahead = jnp.where(
        lax.broadcasted_iota(jnp.int32, (tokens, tokens), 0) < lax.broadcasted_iota(jnp.int32, (tokens, tokens), 1),
        1.0, 0.0,
    ).astype(jnp.bfloat16)
    earlier = jnp.dot(named, ahead, preferred_element_type=jnp.float32)
    row = lax.broadcasted_iota(jnp.int32, (slots_ref.shape[0], tokens), 0).astype(jnp.float32)
    short = row[: rows_ref.shape[0]]
    hit = None
    for k, chosen in enumerate((first, second)):
        rank = jnp.sum(jnp.where(expert == chosen, earlier, 0.0), axis=0, keepdims=True)
        wide = row == chosen.astype(jnp.float32) * stride + rank
        slots_ref[:, k * tokens : (k + 1) * tokens] = jnp.where(wide, 1.0, 0.0).astype(slots_ref.dtype)
        match = short == chosen.astype(jnp.float32) * capacity + rank
        hit = match if hit is None else hit | match
    picks_ref[...] = jnp.where(hit, 1.0, 0.0).astype(picks_ref.dtype)
    block = lax.broadcasted_iota(jnp.int32, (scale_ref.shape[1], step), 0)
    lane = lax.broadcasted_iota(jnp.int32, (scale_ref.shape[1], step), 1) // (width // scale_ref.shape[1])
    per_step = step * scale_ref.shape[1] // width

    def build(piece, carry):
        spread = jnp.where(block == lane + piece * per_step, 1.0, 0.0).astype(jnp.bfloat16)
        scale = jnp.dot(scale_ref[...], spread, preferred_element_type=jnp.float32)
        span = pl.ds(pl.multiple_of(piece * step, step), step)
        value = (stash_ref[:, span].astype(jnp.float32) * scale).astype(jnp.bfloat16)
        placed = jnp.dot(picks_ref[...], value, preferred_element_type=jnp.float32)
        build_ref[:, span] = placed.astype(build_ref.dtype)
        return carry

    lax.fori_loop(0, pieces // 2, build, 0)
    for j in range(1, ys):
        piece = landed(x, y_at(-j), 0)
        moved(own[0], piece, y_send.at[j - 1], y_recv.at[j - 1], y_place(j)).wait_recv()
        for k in range(1, xs):
            send(moved(piece, piece, yx_send.at[j, k - 1], yx_recv.at[j, k - 1], x_place(k)))
    for j in range(1, xs):
        piece = landed(x_at(-j), y, 1)
        moved(own[1], piece, x_send.at[j - 1], x_recv.at[j - 1], x_place(j)).wait_recv()
        for k in range(1, ys):
            send(moved(piece, piece, xy_send.at[j, k - 1], xy_recv.at[j, k - 1], y_place(k)))
    lax.fori_loop(pieces // 2, pieces, build, 0)
    put = pltpu.make_async_copy(build_ref, rows_ref, build_sem)
    put.start()
    for j in range(ys):
        for k in range(1, xs):
            piece = landed(x_at(-k), y_at(-j), 0)
            moved(own[0], piece, yx_send.at[j, k - 1], yx_recv.at[j, k - 1], x_place(k)).wait_recv()
    for j in range(xs):
        for k in range(1, ys):
            piece = landed(x_at(-j), y_at(-k), 1)
            moved(own[1], piece, xy_send.at[j, k - 1], xy_recv.at[j, k - 1], y_place(k)).wait_recv()
    for copy in sends:
        copy.wait_send()
    keep.wait()
    put.wait()


def front(id_rows, stash, scales, w_down, capacity, stride):
    tokens, width = stash.shape
    rows, hidden = w_down.shape
    experts = lax.axis_size(ROW_AXES)
    xs, ys = 2 * lax.axis_size("xhi"), lax.axis_size("y")
    kind = stash.dtype
    vmem = pl.BlockSpec(memory_space=pltpu.VMEM)
    anywhere = pl.BlockSpec(memory_space=pl.ANY)
    semaphores = []
    for shape in ((ys - 1,), (xs - 1,), (ys, xs - 1), (xs, ys - 1)):
        semaphores += [pltpu.SemaphoreType.DMA(shape), pltpu.SemaphoreType.DMA(shape)]
    return pl.pallas_call(
        functools.partial(front_kernel, xs, ys, capacity, stride, 8),
        out_shape=(
            jax.ShapeDtypeStruct((experts * capacity, width), kind),
            jax.ShapeDtypeStruct((2, experts, rows, hidden), kind),
            jax.ShapeDtypeStruct((experts * capacity, tokens), kind),
            jax.ShapeDtypeStruct((experts * stride, 2 * tokens), kind),
        ),
        in_specs=[vmem, vmem, vmem, vmem],
        out_specs=(anywhere, anywhere, vmem, vmem),
        scratch_shapes=[
            pltpu.VMEM((experts * capacity, width), kind),
            pltpu.SemaphoreType.DMA,
            pltpu.SemaphoreType.DMA,
        ] + semaphores,
        compiler_params=pltpu.CompilerParams(
            collective_id=3, has_side_effects=True, vmem_limit_bytes=60 * 1024 * 1024
        ),
        cost_estimate=pl.CostEstimate(flops=20_000_000_000, bytes_accessed=10_000_000, transcendentals=0),
        name="front",
    )(id_rows, stash, scales, w_down)


def relay_kernel(zs, grad_ref, ids_in_ref, gate_ref, weight_ref, slots_ref, out_ref, ids_ref, turn_ref, ids_send, ids_recv,
                 tail_ref, tail_send, tail_recv, tail_sem, slice_ref, wide_ref, pick_ref, stage_ref, back_ref,
                 own_sem, slice_send, slice_recv, weight_sem, weight_send, weight_recv, back_send, back_recv):
    z, xlo, core = ring_place()
    tokens = slice_ref.shape[1]
    depth = slice_ref.shape[2]
    experts_out = out_ref.shape[0]
    mine = lax.axis_index("xhi") * (experts_out // 2) + lax.axis_index("y")

    def row_of(shift):
        return lax.rem(mine + shift, experts_out)

    def row_place(shift):
        row = row_of(shift)
        return {"xhi": row // (experts_out // 2), "y": lax.rem(row, experts_out // 2)}

    experts = weight_ref.shape[1]
    rows = weight_ref.shape[2]
    half = zs // 2
    offsets = []
    for d in range(1, half):
        offsets += [-d, d]
    offsets += [half, 0]
    twin = place(z, xlo, 1 - core)

    def peer(offset):
        return lax.rem(z + offset + zs, zs)

    def mirror(slot):
        return slot if slot >= zs - 2 else slot ^ 1

    greet(
        [place(peer(offset), xlo, core) for offset in offsets[:-1]]
        + [twin]
        + [row_place(shift) for shift in range(1, experts_out)]
    )

    def tail_copy(shift):
        return pltpu.make_async_remote_copy(
            src_ref=tail_ref.at[row_of(shift)],
            dst_ref=out_ref.at[mine],
            send_sem=tail_send.at[shift - 1],
            recv_sem=tail_recv.at[shift - 1],
            device_id=row_place(shift),
            device_id_type=MESH,
        )

    def tail_arrival(shift):
        source = row_of(experts_out - shift)
        return pltpu.make_async_remote_copy(
            src_ref=tail_ref.at[source],
            dst_ref=out_ref.at[source],
            send_sem=tail_send.at[shift - 1],
            recv_sem=tail_recv.at[shift - 1],
            device_id=twin,
            device_id_type=MESH,
        )

    def ids_copy(slot):
        return pltpu.make_async_remote_copy(
            src_ref=ids_in_ref,
            dst_ref=ids_ref.at[mirror(slot)],
            send_sem=ids_send.at[slot],
            recv_sem=ids_recv.at[mirror(slot)],
            device_id=place(peer(offsets[slot]), xlo, core),
            device_id_type=MESH,
        )

    def ids_arrival(slot):
        return pltpu.make_async_remote_copy(
            src_ref=ids_ref.at[slot],
            dst_ref=ids_ref.at[slot],
            send_sem=ids_send.at[slot],
            recv_sem=ids_recv.at[slot],
            device_id=twin,
            device_id_type=MESH,
        )

    def columns(offset):
        return pl.ds(pl.multiple_of(peer(offset) * depth, depth), depth)

    def slice_copy(slot):
        return pltpu.make_async_remote_copy(
            src_ref=grad_ref.at[:, columns(offsets[slot])],
            dst_ref=slice_ref.at[mirror(slot)],
            send_sem=slice_send.at[slot],
            recv_sem=slice_recv.at[mirror(slot)],
            device_id=place(peer(offsets[slot]), xlo, core),
            device_id_type=MESH,
        )

    def back_copy(slot):
        return pltpu.make_async_remote_copy(
            src_ref=stage_ref.at[slot],
            dst_ref=back_ref.at[mirror(slot)],
            send_sem=back_send.at[slot],
            recv_sem=back_recv.at[mirror(slot)],
            device_id=place(peer(offsets[slot]), xlo, core),
            device_id_type=MESH,
        )

    def slice_arrival(slot):
        return pltpu.make_async_remote_copy(
            src_ref=slice_ref.at[slot],
            dst_ref=slice_ref.at[slot],
            send_sem=slice_send.at[slot],
            recv_sem=slice_recv.at[slot],
            device_id=twin,
            device_id_type=MESH,
        )

    def back_arrival(slot):
        return pltpu.make_async_remote_copy(
            src_ref=back_ref.at[slot],
            dst_ref=back_ref.at[slot],
            send_sem=back_send.at[slot],
            recv_sem=back_recv.at[slot],
            device_id=twin,
            device_id_type=MESH,
        )

    def weight_rows(plane, side):
        return wide_ref.at[:, pl.ds(pl.multiple_of((2 * plane + side) * rows, rows), rows), :]

    def weight_copy(plane):
        return pltpu.make_async_remote_copy(
            src_ref=weight_ref.at[plane],
            dst_ref=weight_rows(plane, core),
            send_sem=weight_send.at[plane],
            recv_sem=weight_recv.at[plane],
            device_id=twin,
            device_id_type=MESH,
        )

    def weight_arrival(plane):
        return pltpu.make_async_remote_copy(
            src_ref=weight_ref.at[plane],
            dst_ref=weight_rows(plane, 1 - core),
            send_sem=weight_send.at[plane],
            recv_sem=weight_recv.at[plane],
            device_id=twin,
            device_id_type=MESH,
        )

    keeps = [pltpu.make_async_copy(grad_ref.at[:, columns(0)], slice_ref.at[zs - 1], own_sem)]
    for plane in range(2):
        keeps.append(pltpu.make_async_copy(weight_ref.at[plane], weight_rows(plane, core), weight_sem.at[plane]))
    for slot in range(zs - 1):
        ids_copy(slot).start()
    for slot in range(zs - 1):
        slice_copy(slot).start()
    for plane in range(2):
        weight_copy(plane).start()
    ids_ref[zs - 1] = ids_in_ref[...]
    for keep in keeps:
        keep.start()
    for keep in keeps:
        keep.wait()
    for plane in range(2):
        weight_arrival(plane).wait_recv()
    for pair in range(half):
        for side in range(2):
            slot = 2 * pair + side
            if slot < zs - 1:
                ids_arrival(slot).wait_recv()
                slice_arrival(slot).wait_recv()
        pick_ref[...] = jnp.zeros_like(pick_ref)
        for side in range(2):
            tall = jnp.concatenate([ids_ref[2 * pair + side]] * (tokens // ids_ref.shape[1]), axis=0)
            turn_ref[pl.ds(side * tokens, tokens), :] = tall.T

        def per_expert(e, carry):
            both = slice_ref[pl.ds(2 * pair, 2)].reshape(2 * tokens, depth)
            dense = jnp.dot(both, wide_ref[e], preferred_element_type=jnp.float32)
            for k in range(2):
                pick_ref[k] = jnp.where(turn_ref[:, k : k + 1] == e, dense, pick_ref[k])
            return carry

        lax.fori_loop(0, experts, per_expert, 0)
        for side in range(2):
            slot = 2 * pair + side
            for k in range(2):
                stage_ref[slot, k] = pick_ref[k, pl.ds(side * tokens, tokens), :].astype(stage_ref.dtype)
            if slot < zs - 1:
                back_copy(slot).start()
    total = stage_ref[zs - 1].astype(jnp.float32)
    for slot in range(zs - 1):
        back_arrival(slot).wait_recv()
        total = total + back_ref[slot].astype(jnp.float32)
    weighted = [(total[k] * gate_ref[:, k : k + 1]).astype(tail_ref.dtype) for k in range(2)]
    placed = jnp.dot(slots_ref[...], jnp.concatenate(weighted, axis=0), preferred_element_type=jnp.float32)
    tail_ref[...] = placed.astype(tail_ref.dtype).reshape(tail_ref.shape)
    for shift in range(1, experts_out):
        tail_copy(shift).start()
    keep_tail = pltpu.make_async_copy(tail_ref.at[mine], out_ref.at[mine], tail_sem)
    keep_tail.start()
    for slot in range(zs - 1):
        ids_copy(slot).wait_send()
        slice_copy(slot).wait_send()
        back_copy(slot).wait_send()
    for plane in range(2):
        weight_copy(plane).wait_send()
    for shift in range(1, experts_out):
        tail_arrival(shift).wait_recv()
        tail_copy(shift).wait_send()
    keep_tail.wait()


def relay(out_grad, route_ids, gates, weights, slots, zs):
    tokens, feature_width = out_grad.shape
    planes, experts, rows, hidden = weights.shape
    depth = feature_width // zs
    tail_rows = slots.shape[0] // experts
    kind = out_grad.dtype
    vmem = pl.BlockSpec(memory_space=pltpu.VMEM)
    anywhere = pl.BlockSpec(memory_space=pl.ANY)
    pairs = pltpu.SemaphoreType.DMA((zs - 1,))
    others = pltpu.SemaphoreType.DMA((experts - 1,))
    return pl.pallas_call(
        functools.partial(relay_kernel, zs),
        out_shape=jax.ShapeDtypeStruct((experts, tail_rows, hidden), kind),
        in_specs=[anywhere, vmem, vmem, anywhere, vmem],
        out_specs=anywhere,
        scratch_shapes=[
            pltpu.VMEM((zs,) + route_ids.shape, route_ids.dtype),
            pltpu.VMEM((2 * tokens, tokens), route_ids.dtype),
            pairs,
            pairs,
            pltpu.VMEM((experts, tail_rows, hidden), kind),
            others,
            others,
            pltpu.SemaphoreType.DMA,
            pltpu.VMEM((zs, tokens, depth), kind),
            pltpu.VMEM((experts, 2 * planes * rows, hidden), kind),
            pltpu.VMEM((2, 2 * tokens, hidden), jnp.float32),
            pltpu.VMEM((zs, 2, tokens, hidden), kind),
            pltpu.VMEM((zs - 1, 2, tokens, hidden), kind),
            pltpu.SemaphoreType.DMA,
            pairs,
            pairs,
            pltpu.SemaphoreType.DMA((2,)),
            pltpu.SemaphoreType.DMA((2,)),
            pltpu.SemaphoreType.DMA((2,)),
            pairs,
            pairs,
        ],
        compiler_params=pltpu.CompilerParams(
            collective_id=1, has_side_effects=True, vmem_limit_bytes=24 * 1024 * 1024
        ),
        cost_estimate=pl.CostEstimate(flops=40_000_000_000, bytes_accessed=7_000_000, transcendentals=0),
        name="relay",
    )(out_grad, route_ids, gates, weights, slots)


def on_device(stash, scales, out_grad, route_ids, gates, w_gate_up, w_down):
    tokens, feature_width = stash.shape
    hidden = w_down.shape[2]
    experts = lax.axis_size(ROW_AXES)
    dp_count = lax.axis_size(COLUMN_AXES)
    capacity = min(tokens, 7 * tokens // (2 * experts))
    stride = -(-capacity // 16) * 16
    id_rows = jnp.pad(route_ids.T, ((0, 6), (0, 0)))
    sent_x, weights, picks, slots = front(id_rows, stash, scales, w_down[0], capacity, stride)
    weight_in = w_gate_up[0]
    zs = lax.axis_size("z")
    features = exchange(sent_x, experts, capacity)
    got_hidden = relay(out_grad, id_rows, gates, weights, slots, zs)
    back_hidden = got_hidden[:, :capacity].reshape(experts * capacity, hidden).astype(jnp.float32)
    gate_up = jnp.dot(features, weight_in, preferred_element_type=jnp.float32)
    hidden_grad = gated_backward(gate_up, back_hidden)
    slot_grads = lax.dot_general(
        hidden_grad, weight_in, (((1,), (1,)), ((), ())), preferred_element_type=jnp.float32
    ).astype(jnp.bfloat16)
    returned = exchange(slot_grads, experts, capacity)
    input_grad = lax.dot_general(
        picks, returned, (((0,), (0,)), ((), ())), preferred_element_type=jnp.float32
    ).astype(jnp.bfloat16)
    local_rows = feature_width // dp_count
    partial_grad = lax.dot_general(
        features, hidden_grad, (((0,), (0,)), ((), ())), preferred_element_type=jnp.float32
    ).astype(jnp.bfloat16)
    grad_gate_up = reduce_rows(partial_grad, dp_count, 2).reshape(1, local_rows, 2 * hidden)
    return (input_grad, grad_gate_up)


def solution(mesh):
    dp_count, experts = mesh.devices.shape
    split = Mesh(
        mesh.devices.reshape(dp_count // 4, 2, 2, 2, experts // 2), COLUMN_AXES + ROW_AXES
    )
    tokens = P(COLUMN_AXES + ROW_AXES, None)
    placed = (tokens, tokens, tokens, tokens, tokens, P(ROW_AXES, None, None), P(ROW_AXES, COLUMN_AXES, None))
    return jax.shard_map(
        on_device,
        mesh=split,
        in_specs=placed,
        out_specs=(tokens, P(ROW_AXES, COLUMN_AXES, None)),
        check_vma=False,
    )
```

```python
import functools

import jax
import jax.numpy as jnp
from jax import lax
from jax.experimental import pallas as pl
from jax.experimental.pallas import tpu as pltpu
from jax.sharding import Mesh
from jax.sharding import PartitionSpec as P

MESH = pl.DeviceIdType.MESH
COLUMN_AXES = ("z", "xlo", "core")
ROW_AXES = ("xhi", "y")


def ring_place():
    return lax.axis_index("z"), lax.axis_index("xlo"), lax.axis_index("core")


def place(z, xlo, core):
    return {"z": z, "xlo": xlo, "core": core}


def greet(partners):
    barrier = pltpu.get_barrier_semaphore()
    for partner in partners:
        pl.semaphore_signal(barrier, inc=1, device_id=partner, device_id_type=MESH)
    pl.semaphore_wait(barrier, len(partners))


def reduce_kernel(zs, subs, part_ref, out_ref, core_ref, ring_ref, stage_ref, side_ref,
                  core_send, core_recv, ring_send, ring_recv, side_send, side_recv):
    z, xlo, core = ring_place()
    rows = part_ref.shape[1]
    step_rows = rows // subs

    def at(zz, xx, cc):
        return zz * 4 + xx * 2 + cc

    up, down = lax.rem(z + 1, zs), lax.rem(z + zs - 1, zs)
    to_up, to_down = place(up, xlo, core), place(down, xlo, core)
    to_side, to_twin = place(z, 1 - xlo, core), place(z, xlo, 1 - core)
    greet((to_up, to_down, to_side, to_twin))

    def owner(way, step):
        return lax.rem(z + 2 * zs - 1 - step, zs) if way == 0 else lax.rem(z + 1 + step, zs)

    def core_copy(way, step):
        piece = owner(way, step)
        return pltpu.make_async_remote_copy(
            src_ref=part_ref.at[at(piece, way, 1 - core)],
            dst_ref=core_ref.at[way, step],
            send_sem=core_send.at[way, step],
            recv_sem=core_recv.at[way, step],
            device_id=to_twin,
            device_id_type=MESH,
        )

    def ring_copy(way, step, sub):
        return pltpu.make_async_remote_copy(
            src_ref=stage_ref.at[way, step, sub],
            dst_ref=ring_ref.at[way, step, sub],
            send_sem=ring_send.at[way, step, sub],
            recv_sem=ring_recv.at[way, step, sub],
            device_id=to_up if way == 0 else to_down,
            device_id_type=MESH,
        )

    def side_copy(sub):
        return pltpu.make_async_remote_copy(
            src_ref=stage_ref.at[1 - xlo, zs - 1, sub],
            dst_ref=side_ref.at[sub],
            send_sem=side_send.at[sub],
            recv_sem=side_recv.at[sub],
            device_id=to_side,
            device_id_type=MESH,
        )

    for step in range(zs):
        for way in range(2):
            core_copy(way, step).start()
    for step in range(zs):
        for sub in range(subs):
            for way in range(2):
                if sub == 0:
                    core_copy(way, step).wait_recv()
                piece = at(owner(way, step), way, core)
                span = pl.ds(sub * step_rows, step_rows)
                value = part_ref[piece, span, :].astype(jnp.float32) + core_ref[way, step, span, :].astype(jnp.float32)
                if step > 0:
                    ring_copy(way, step - 1, sub).wait_recv()
                    value = value + ring_ref[way, step - 1, sub].astype(jnp.float32)
                stage_ref[way, step, sub] = value.astype(stage_ref.dtype)
                if step < zs - 1:
                    ring_copy(way, step, sub).start()
        if step == zs - 1:
            for sub in range(subs):
                side_copy(sub).start()
    share = 1.0 / (4 * zs)
    for sub in range(subs):
        side_copy(sub).wait_recv()
        span = pl.ds(sub * step_rows, step_rows)
        total = stage_ref[xlo, zs - 1, sub].astype(jnp.float32) + side_ref[sub].astype(jnp.float32)
        out_ref[span, :] = total * share
    for step in range(zs):
        for way in range(2):
            core_copy(way, step).wait_send()
            for sub in range(subs):
                if step < zs - 1:
                    ring_copy(way, step, sub).wait_send()
    for sub in range(subs):
        side_copy(sub).wait_send()


def reduce_rows(part, dp_count, collective_id, subs=2):
    zs = dp_count // 4
    width = part.shape[1]
    rows = part.shape[0] // dp_count
    kind = part.dtype
    return pl.pallas_call(
        functools.partial(reduce_kernel, zs, subs),
        out_shape=jax.ShapeDtypeStruct((rows, width), jnp.float32),
        in_specs=[pl.BlockSpec(memory_space=pltpu.VMEM)],
        out_specs=pl.BlockSpec(memory_space=pltpu.VMEM),
        scratch_shapes=[
            pltpu.VMEM((2, zs, rows, width), kind),
            pltpu.VMEM((2, zs - 1, subs, rows // subs, width), kind),
            pltpu.VMEM((2, zs, subs, rows // subs, width), kind),
            pltpu.VMEM((subs, rows // subs, width), kind),
            pltpu.SemaphoreType.DMA((2, zs)),
            pltpu.SemaphoreType.DMA((2, zs)),
            pltpu.SemaphoreType.DMA((2, zs - 1, subs)),
            pltpu.SemaphoreType.DMA((2, zs - 1, subs)),
            pltpu.SemaphoreType.DMA((subs,)),
            pltpu.SemaphoreType.DMA((subs,)),
        ],
        compiler_params=pltpu.CompilerParams(
            collective_id=collective_id, has_side_effects=True, vmem_limit_bytes=32 * 1024 * 1024
        ),
        cost_estimate=pl.CostEstimate(flops=40_000_000_000, bytes_accessed=7_000_000, transcendentals=0),
        name="reduce_rows",
    )(part.reshape(dp_count, rows, width))


def gated_backward(gate_up, back_hidden):
    hidden = back_hidden.shape[1]
    gate_value = gate_up[:, :hidden]
    up_value = gate_up[:, hidden:]
    sigmoid_gate = jax.nn.sigmoid(gate_value)
    grad_gate = back_hidden * up_value * sigmoid_gate * (1.0 + gate_value * (1.0 - sigmoid_gate))
    grad_up = back_hidden * gate_value * sigmoid_gate
    return jnp.concatenate([grad_gate, grad_up], axis=1).astype(jnp.bfloat16)


def exchange(rows, experts, capacity):
    width = rows.shape[1]
    moved = lax.all_to_all(
        rows.reshape(experts, capacity, width), ROW_AXES, split_axis=0, concat_axis=0, tiled=True
    )
    return moved.reshape(experts * capacity, width)


def ring_offsets(zs):
    offsets = []
    for d in range(1, zs // 2):
        offsets += [-d, d]
    return offsets + [zs // 2, 0]


def near_slots(zs):
    return min(4, zs - 2)


def front_kernel(zs, xs, ys, capacity, stride, pieces, ids_ref, stash_ref, scale_ref, weight_ref, grad_ref,
                 rows_ref, plane_ref, picks_ref, slots_ref, tile_ref, near_ref, near_send, near_recv,
                 build_ref, build_sem, keep_sem, y_send, y_recv, x_send, x_recv, yx_send, yx_recv, xy_send, xy_recv):
    xlo, xhi, y = lax.axis_index("xlo"), lax.axis_index("xhi"), lax.axis_index("y")
    x = xhi * 2 + xlo
    z = lax.axis_index("z")
    tokens, width = stash_ref.shape
    depth = width // zs
    near = near_slots(zs)
    offsets = ring_offsets(zs)
    half = weight_ref.shape[0] // 2
    step = width // pieces

    def x_at(shift):
        return lax.rem(x + shift + xs, xs)

    def y_at(shift):
        return lax.rem(y + shift + ys, ys)

    def x_place(shift):
        return {"xlo": lax.rem(x_at(shift), 2), "xhi": x_at(shift) // 2}

    def y_place(shift):
        return {"y": y_at(shift)}

    def landed(xx, yy, part):
        return plane_ref.at[lax.rem(xx, 2), (xx // 2) * ys + yy, pl.ds(part * half, half), :]

    def moved(source, target, send, recv, device):
        return pltpu.make_async_remote_copy(
            src_ref=source, dst_ref=target, send_sem=send, recv_sem=recv, device_id=device, device_id_type=MESH
        )

    def z_at(slot):
        return lax.rem(z + offsets[slot] + zs, zs)

    greet(
        [x_place(k) for k in range(1, xs)]
        + [y_place(k) for k in range(1, ys)]
        + [{"z": z_at(slot)} for slot in range(near)]
    )
    own = [weight_ref.at[pl.ds(part * half, half), :] for part in range(2)]
    keep = pltpu.make_async_copy(weight_ref, plane_ref.at[xlo, xhi * ys + y], keep_sem)
    keep.start()
    sends, waits = [], []

    def send(copy):
        copy.start()
        sends.append(copy)

    for k in range(1, ys):
        send(moved(own[0], landed(x, y, 0), y_send.at[k - 1], y_recv.at[k - 1], y_place(k)))
    for k in range(1, xs):
        send(moved(own[1], landed(x, y, 1), x_send.at[k - 1], x_recv.at[k - 1], x_place(k)))
    for k in range(1, xs):
        send(moved(own[0], landed(x, y, 0), yx_send.at[0, k - 1], yx_recv.at[0, k - 1], x_place(k)))
    for k in range(1, ys):
        send(moved(own[1], landed(x, y, 1), xy_send.at[0, k - 1], xy_recv.at[0, k - 1], y_place(k)))

    for slot in range(near):
        columns = grad_ref.at[:, pl.ds(pl.multiple_of(z_at(slot) * depth, depth), depth)]
        send(moved(columns, near_ref.at[slot ^ 1], near_send.at[slot], near_recv.at[slot ^ 1], {"z": z_at(slot)}))

    expert = lax.broadcasted_iota(jnp.int32, tile_ref.shape, 0)
    first, second = ids_ref[0:1, :], ids_ref[1:2, :]
    tile_ref[...] = jnp.where(expert == 0, first, second)
    named = jnp.where((expert == first) | (expert == second), 1.0, 0.0).astype(jnp.bfloat16)
    ahead = jnp.where(
        lax.broadcasted_iota(jnp.int32, (tokens, tokens), 0) < lax.broadcasted_iota(jnp.int32, (tokens, tokens), 1),
        1.0, 0.0,
    ).astype(jnp.bfloat16)
    earlier = jnp.dot(named, ahead, preferred_element_type=jnp.float32)
    row = lax.broadcasted_iota(jnp.int32, (slots_ref.shape[0], tokens), 0).astype(jnp.float32)
    short = row[: rows_ref.shape[0]]
    hit = None
    for k, chosen in enumerate((first, second)):
        rank = jnp.sum(jnp.where(expert == chosen, earlier, 0.0), axis=0, keepdims=True)
        wide = row == chosen.astype(jnp.float32) * stride + rank
        slots_ref[:, k * tokens : (k + 1) * tokens] = jnp.where(wide, 1.0, 0.0).astype(slots_ref.dtype)
        match = short == chosen.astype(jnp.float32) * capacity + rank
        hit = match if hit is None else hit | match
    picks_ref[...] = jnp.where(hit, 1.0, 0.0).astype(picks_ref.dtype)
    blocks = scale_ref.shape[0]
    block = lax.broadcasted_iota(jnp.int32, (blocks, step), 0)
    lane = lax.broadcasted_iota(jnp.int32, (blocks, step), 1) // (width // blocks)
    per_step = step * blocks // width

    def build(piece, carry):
        spread = jnp.where(block == lane + piece * per_step, 1.0, 0.0).astype(jnp.bfloat16)
        scale = lax.dot_general(
            scale_ref[...], spread, (((0,), (0,)), ((), ())), preferred_element_type=jnp.float32
        )
        span = pl.ds(pl.multiple_of(piece * step, step), step)
        value = (stash_ref[:, span].astype(jnp.float32) * scale).astype(jnp.bfloat16)
        placed = jnp.dot(picks_ref[...], value, preferred_element_type=jnp.float32)
        build_ref[:, span] = placed.astype(build_ref.dtype)
        return carry

    lax.fori_loop(0, pieces // 2, build, 0)
    for j in range(1, ys):
        piece = landed(x, y_at(-j), 0)
        moved(own[0], piece, y_send.at[j - 1], y_recv.at[j - 1], y_place(j)).wait_recv()
        for k in range(1, xs):
            send(moved(piece, piece, yx_send.at[j, k - 1], yx_recv.at[j, k - 1], x_place(k)))
    for j in range(1, xs):
        piece = landed(x_at(-j), y, 1)
        moved(own[1], piece, x_send.at[j - 1], x_recv.at[j - 1], x_place(j)).wait_recv()
        for k in range(1, ys):
            send(moved(piece, piece, xy_send.at[j, k - 1], xy_recv.at[j, k - 1], y_place(k)))
    lax.fori_loop(pieces // 2, pieces, build, 0)
    put = pltpu.make_async_copy(build_ref, rows_ref, build_sem)
    put.start()
    for j in range(ys):
        for k in range(1, xs):
            piece = landed(x_at(-k), y_at(-j), 0)
            moved(own[0], piece, yx_send.at[j, k - 1], yx_recv.at[j, k - 1], x_place(k)).wait_recv()
    for j in range(xs):
        for k in range(1, ys):
            piece = landed(x_at(-j), y_at(-k), 1)
            moved(own[1], piece, xy_send.at[j, k - 1], xy_recv.at[j, k - 1], y_place(k)).wait_recv()
    for slot in range(near):
        landing = near_ref.at[slot]
        moved(landing, landing, near_send.at[slot], near_recv.at[slot], {"z": z_at(slot)}).wait_recv()
    for copy in sends:
        copy.wait_send()
    keep.wait()
    put.wait()


def front(id_rows, stash, scale_rows, w_down, out_grad, capacity, stride):
    tokens, width = stash.shape
    rows, hidden = w_down.shape
    experts = lax.axis_size(ROW_AXES)
    zs, xs, ys = lax.axis_size("z"), 2 * lax.axis_size("xhi"), lax.axis_size("y")
    near = near_slots(zs)
    kind = stash.dtype
    vmem = pl.BlockSpec(memory_space=pltpu.VMEM)
    anywhere = pl.BlockSpec(memory_space=pl.ANY)
    semaphores = []
    for shape in ((ys - 1,), (xs - 1,), (ys, xs - 1), (xs, ys - 1)):
        semaphores += [pltpu.SemaphoreType.DMA(shape), pltpu.SemaphoreType.DMA(shape)]
    return pl.pallas_call(
        functools.partial(front_kernel, zs, xs, ys, capacity, stride, 8),
        out_shape=(
            jax.ShapeDtypeStruct((experts * capacity, width), kind),
            jax.ShapeDtypeStruct((2, experts, rows, hidden), kind),
            jax.ShapeDtypeStruct((experts * capacity, tokens), kind),
            jax.ShapeDtypeStruct((experts * stride, 2 * tokens), kind),
            jax.ShapeDtypeStruct((8, tokens), id_rows.dtype),
            jax.ShapeDtypeStruct((near, tokens, width // zs), kind),
        ),
        in_specs=[vmem, vmem, vmem, vmem, anywhere],
        out_specs=(anywhere, anywhere, vmem, vmem, vmem, anywhere),
        scratch_shapes=[
            pltpu.SemaphoreType.DMA((near,)),
            pltpu.SemaphoreType.DMA((near,)),
            pltpu.VMEM((experts * capacity, width), kind),
            pltpu.SemaphoreType.DMA,
            pltpu.SemaphoreType.DMA,
        ] + semaphores,
        compiler_params=pltpu.CompilerParams(
            collective_id=3, has_side_effects=True, vmem_limit_bytes=60 * 1024 * 1024
        ),
        cost_estimate=pl.CostEstimate(flops=20_000_000_000, bytes_accessed=10_000_000, transcendentals=0),
        name="front",
    )(id_rows, stash, scale_rows, w_down, out_grad)


def relay_kernel(zs, grad_ref, near_ref, ids_in_ref, gate_ref, weight_ref, slots_ref, out_ref, ids_ref, turn_ref, ids_send, ids_recv,
                 tail_ref, tail_send, tail_recv, tail_sem, slice_ref, wide_ref, pick_ref, stage_ref, back_ref,
                 own_sem, near_sem, slice_send, slice_recv, weight_sem, weight_send, weight_recv, back_send, back_recv):
    z, xlo, core = ring_place()
    tokens = slice_ref.shape[1]
    depth = slice_ref.shape[2]
    experts_out = out_ref.shape[0]
    mine = lax.axis_index("xhi") * (experts_out // 2) + lax.axis_index("y")

    def row_of(shift):
        return lax.rem(mine + shift, experts_out)

    def row_place(shift):
        row = row_of(shift)
        return {"xhi": row // (experts_out // 2), "y": lax.rem(row, experts_out // 2)}

    experts = weight_ref.shape[1]
    rows = weight_ref.shape[2]
    half = zs // 2
    offsets = ring_offsets(zs)
    near = near_slots(zs)
    twin = place(z, xlo, 1 - core)

    def peer(offset):
        return lax.rem(z + offset + zs, zs)

    def mirror(slot):
        return slot if slot >= zs - 2 else slot ^ 1

    greet(
        [place(peer(offset), xlo, core) for offset in offsets[:-1]]
        + [twin]
        + [row_place(shift) for shift in range(1, experts_out)]
    )

    def tail_copy(shift):
        return pltpu.make_async_remote_copy(
            src_ref=tail_ref.at[row_of(shift)],
            dst_ref=out_ref.at[mine],
            send_sem=tail_send.at[shift - 1],
            recv_sem=tail_recv.at[shift - 1],
            device_id=row_place(shift),
            device_id_type=MESH,
        )

    def tail_arrival(shift):
        source = row_of(experts_out - shift)
        return pltpu.make_async_remote_copy(
            src_ref=tail_ref.at[source],
            dst_ref=out_ref.at[source],
            send_sem=tail_send.at[shift - 1],
            recv_sem=tail_recv.at[shift - 1],
            device_id=twin,
            device_id_type=MESH,
        )

    def ids_copy(slot):
        return pltpu.make_async_remote_copy(
            src_ref=ids_in_ref,
            dst_ref=ids_ref.at[mirror(slot)],
            send_sem=ids_send.at[slot],
            recv_sem=ids_recv.at[mirror(slot)],
            device_id=place(peer(offsets[slot]), xlo, core),
            device_id_type=MESH,
        )

    def ids_arrival(slot):
        return pltpu.make_async_remote_copy(
            src_ref=ids_ref.at[slot],
            dst_ref=ids_ref.at[slot],
            send_sem=ids_send.at[slot],
            recv_sem=ids_recv.at[slot],
            device_id=twin,
            device_id_type=MESH,
        )

    def columns(offset):
        return pl.ds(pl.multiple_of(peer(offset) * depth, depth), depth)

    def slice_copy(slot):
        return pltpu.make_async_remote_copy(
            src_ref=grad_ref.at[:, columns(offsets[slot])],
            dst_ref=slice_ref.at[mirror(slot)],
            send_sem=slice_send.at[slot],
            recv_sem=slice_recv.at[mirror(slot)],
            device_id=place(peer(offsets[slot]), xlo, core),
            device_id_type=MESH,
        )

    def back_copy(slot):
        return pltpu.make_async_remote_copy(
            src_ref=stage_ref.at[slot],
            dst_ref=back_ref.at[mirror(slot)],
            send_sem=back_send.at[slot],
            recv_sem=back_recv.at[mirror(slot)],
            device_id=place(peer(offsets[slot]), xlo, core),
            device_id_type=MESH,
        )

    def slice_arrival(slot):
        return pltpu.make_async_remote_copy(
            src_ref=slice_ref.at[slot],
            dst_ref=slice_ref.at[slot],
            send_sem=slice_send.at[slot],
            recv_sem=slice_recv.at[slot],
            device_id=twin,
            device_id_type=MESH,
        )

    def back_arrival(slot):
        return pltpu.make_async_remote_copy(
            src_ref=back_ref.at[slot],
            dst_ref=back_ref.at[slot],
            send_sem=back_send.at[slot],
            recv_sem=back_recv.at[slot],
            device_id=twin,
            device_id_type=MESH,
        )

    def weight_rows(plane, side):
        return wide_ref.at[:, pl.ds(pl.multiple_of((2 * plane + side) * rows, rows), rows), :]

    def weight_copy(plane):
        return pltpu.make_async_remote_copy(
            src_ref=weight_ref.at[plane],
            dst_ref=weight_rows(plane, core),
            send_sem=weight_send.at[plane],
            recv_sem=weight_recv.at[plane],
            device_id=twin,
            device_id_type=MESH,
        )

    def weight_arrival(plane):
        return pltpu.make_async_remote_copy(
            src_ref=weight_ref.at[plane],
            dst_ref=weight_rows(plane, 1 - core),
            send_sem=weight_send.at[plane],
            recv_sem=weight_recv.at[plane],
            device_id=twin,
            device_id_type=MESH,
        )

    keeps = [pltpu.make_async_copy(grad_ref.at[:, columns(0)], slice_ref.at[zs - 1], own_sem)]
    keeps.append(pltpu.make_async_copy(near_ref, slice_ref.at[pl.ds(0, near)], near_sem))
    for plane in range(2):
        keeps.append(pltpu.make_async_copy(weight_ref.at[plane], weight_rows(plane, core), weight_sem.at[plane]))
    for slot in range(zs - 1):
        ids_copy(slot).start()
    for slot in range(near, zs - 1):
        slice_copy(slot).start()
    for plane in range(2):
        weight_copy(plane).start()
    ids_ref[zs - 1] = ids_in_ref[...]
    for keep in keeps:
        keep.start()
    for keep in keeps:
        keep.wait()
    for plane in range(2):
        weight_arrival(plane).wait_recv()
    for pair in range(half):
        for side in range(2):
            slot = 2 * pair + side
            if slot < zs - 1:
                ids_arrival(slot).wait_recv()
                if slot >= near:
                    slice_arrival(slot).wait_recv()
        pick_ref[...] = jnp.zeros_like(pick_ref)
        for side in range(2):
            tall = jnp.concatenate([ids_ref[2 * pair + side]] * (tokens // ids_ref.shape[1]), axis=0)
            turn_ref[pl.ds(side * tokens, tokens), :] = tall.T

        def per_expert(e, carry):
            both = slice_ref[pl.ds(2 * pair, 2)].reshape(2 * tokens, depth)
            dense = jnp.dot(both, wide_ref[e], preferred_element_type=jnp.float32)
            for k in range(2):
                pick_ref[k] = jnp.where(turn_ref[:, k : k + 1] == e, dense, pick_ref[k])
            return carry

        lax.fori_loop(0, experts, per_expert, 0)
        for side in range(2):
            slot = 2 * pair + side
            for k in range(2):
                stage_ref[slot, k] = pick_ref[k, pl.ds(side * tokens, tokens), :].astype(stage_ref.dtype)
            if slot < zs - 1:
                back_copy(slot).start()
    total = stage_ref[zs - 1].astype(jnp.float32)
    for slot in range(zs - 1):
        back_arrival(slot).wait_recv()
        total = total + back_ref[slot].astype(jnp.float32)
    weighted = [(total[k] * gate_ref[:, k : k + 1]).astype(tail_ref.dtype) for k in range(2)]
    placed = jnp.dot(slots_ref[...], jnp.concatenate(weighted, axis=0), preferred_element_type=jnp.float32)
    tail_ref[...] = placed.astype(tail_ref.dtype).reshape(tail_ref.shape)
    for shift in range(1, experts_out):
        tail_copy(shift).start()
    keep_tail = pltpu.make_async_copy(tail_ref.at[mine], out_ref.at[mine], tail_sem)
    keep_tail.start()
    for slot in range(zs - 1):
        ids_copy(slot).wait_send()
        if slot >= near:
            slice_copy(slot).wait_send()
        back_copy(slot).wait_send()
    for plane in range(2):
        weight_copy(plane).wait_send()
    for shift in range(1, experts_out):
        tail_arrival(shift).wait_recv()
        tail_copy(shift).wait_send()
    keep_tail.wait()


def relay(out_grad, near, route_ids, gates, weights, slots, zs):
    tokens, feature_width = out_grad.shape
    planes, experts, rows, hidden = weights.shape
    depth = feature_width // zs
    tail_rows = slots.shape[0] // experts
    kind = out_grad.dtype
    vmem = pl.BlockSpec(memory_space=pltpu.VMEM)
    anywhere = pl.BlockSpec(memory_space=pl.ANY)
    pairs = pltpu.SemaphoreType.DMA((zs - 1,))
    others = pltpu.SemaphoreType.DMA((experts - 1,))
    return pl.pallas_call(
        functools.partial(relay_kernel, zs),
        out_shape=jax.ShapeDtypeStruct((experts, tail_rows, hidden), kind),
        in_specs=[anywhere, anywhere, vmem, vmem, anywhere, vmem],
        out_specs=anywhere,
        scratch_shapes=[
            pltpu.VMEM((zs,) + route_ids.shape, route_ids.dtype),
            pltpu.VMEM((2 * tokens, tokens), route_ids.dtype),
            pairs,
            pairs,
            pltpu.VMEM((experts, tail_rows, hidden), kind),
            others,
            others,
            pltpu.SemaphoreType.DMA,
            pltpu.VMEM((zs, tokens, depth), kind),
            pltpu.VMEM((experts, 2 * planes * rows, hidden), kind),
            pltpu.VMEM((2, 2 * tokens, hidden), jnp.float32),
            pltpu.VMEM((zs, 2, tokens, hidden), kind),
            pltpu.VMEM((zs - 1, 2, tokens, hidden), kind),
            pltpu.SemaphoreType.DMA,
            pltpu.SemaphoreType.DMA,
            pairs,
            pairs,
            pltpu.SemaphoreType.DMA((2,)),
            pltpu.SemaphoreType.DMA((2,)),
            pltpu.SemaphoreType.DMA((2,)),
            pairs,
            pairs,
        ],
        compiler_params=pltpu.CompilerParams(
            collective_id=1, has_side_effects=True, vmem_limit_bytes=24 * 1024 * 1024
        ),
        cost_estimate=pl.CostEstimate(flops=40_000_000_000, bytes_accessed=7_000_000, transcendentals=0),
        name="relay",
    )(out_grad, near, route_ids, gates, weights, slots)


def on_device(stash, scales, out_grad, route_ids, gates, w_gate_up, w_down):
    tokens, feature_width = stash.shape
    hidden = w_down.shape[2]
    experts = lax.axis_size(ROW_AXES)
    dp_count = lax.axis_size(COLUMN_AXES)
    capacity = min(tokens, 7 * tokens // (2 * experts))
    stride = -(-capacity // 16) * 16
    sent_x, weights, picks, slots, id_rows, near = front(
        route_ids.T, stash, scales.T, w_down[0], out_grad, capacity, stride
    )
    weight_in = w_gate_up[0]
    zs = lax.axis_size("z")
    features = exchange(sent_x, experts, capacity)
    got_hidden = relay(out_grad, near, id_rows, gates, weights, slots, zs)
    back_hidden = got_hidden[:, :capacity].reshape(experts * capacity, hidden).astype(jnp.float32)
    gate_up = jnp.dot(features, weight_in, preferred_element_type=jnp.float32)
    hidden_grad = gated_backward(gate_up, back_hidden)
    slot_grads = lax.dot_general(
        hidden_grad, weight_in, (((1,), (1,)), ((), ())), preferred_element_type=jnp.float32
    ).astype(jnp.bfloat16)
    returned = exchange(slot_grads, experts, capacity)
    input_grad = lax.dot_general(
        picks, returned, (((0,), (0,)), ((), ())), preferred_element_type=jnp.float32
    ).astype(jnp.bfloat16)
    local_rows = feature_width // dp_count
    partial_grad = lax.dot_general(
        features, hidden_grad, (((0,), (0,)), ((), ())), preferred_element_type=jnp.float32
    ).astype(jnp.bfloat16)
    grad_gate_up = reduce_rows(partial_grad, dp_count, 2).reshape(1, local_rows, 2 * hidden)
    return (input_grad, grad_gate_up)


def solution(mesh):
    dp_count, experts = mesh.devices.shape
    split = Mesh(
        mesh.devices.reshape(dp_count // 4, 2, 2, 2, experts // 2), COLUMN_AXES + ROW_AXES
    )
    tokens = P(COLUMN_AXES + ROW_AXES, None)
    placed = (tokens, tokens, tokens, tokens, tokens, P(ROW_AXES, None, None), P(ROW_AXES, COLUMN_AXES, None))
    return jax.shard_map(
        on_device,
        mesh=split,
        in_specs=placed,
        out_specs=(tokens, P(ROW_AXES, COLUMN_AXES, None)),
        check_vma=False,
    )
```

```python
import functools

import jax
import jax.numpy as jnp
from jax import lax
from jax.experimental import pallas as pl
from jax.experimental.pallas import tpu as pltpu
from jax.sharding import Mesh
from jax.sharding import PartitionSpec as P

MESH = pl.DeviceIdType.MESH
COLUMN_AXES = ("z", "xlo", "core")
ROW_AXES = ("xhi", "y")


def ring_place():
    return lax.axis_index("z"), lax.axis_index("xlo"), lax.axis_index("core")


def place(z, xlo, core):
    return {"z": z, "xlo": xlo, "core": core}


def greet(partners):
    barrier = pltpu.get_barrier_semaphore()
    for partner in partners:
        pl.semaphore_signal(barrier, inc=1, device_id=partner, device_id_type=MESH)
    pl.semaphore_wait(barrier, len(partners))


def reduce_kernel(zs, subs, part_ref, out_ref, core_ref, ring_ref, stage_ref, side_ref,
                  core_send, core_recv, ring_send, ring_recv, side_send, side_recv):
    z, xlo, core = ring_place()
    rows = part_ref.shape[1]
    step_rows = rows // subs

    def at(zz, xx, cc):
        return zz * 4 + xx * 2 + cc

    up, down = lax.rem(z + 1, zs), lax.rem(z + zs - 1, zs)
    to_up, to_down = place(up, xlo, core), place(down, xlo, core)
    to_side, to_twin = place(z, 1 - xlo, core), place(z, xlo, 1 - core)
    greet((to_up, to_down, to_side, to_twin))

    def owner(way, step):
        return lax.rem(z + 2 * zs - 1 - step, zs) if way == 0 else lax.rem(z + 1 + step, zs)

    def core_copy(way, step):
        piece = owner(way, step)
        return pltpu.make_async_remote_copy(
            src_ref=part_ref.at[at(piece, way, 1 - core)],
            dst_ref=core_ref.at[way, step],
            send_sem=core_send.at[way, step],
            recv_sem=core_recv.at[way, step],
            device_id=to_twin,
            device_id_type=MESH,
        )

    def ring_copy(way, step, sub):
        return pltpu.make_async_remote_copy(
            src_ref=stage_ref.at[way, step, sub],
            dst_ref=ring_ref.at[way, step, sub],
            send_sem=ring_send.at[way, step, sub],
            recv_sem=ring_recv.at[way, step, sub],
            device_id=to_up if way == 0 else to_down,
            device_id_type=MESH,
        )

    def side_copy(sub):
        return pltpu.make_async_remote_copy(
            src_ref=stage_ref.at[1 - xlo, zs - 1, sub],
            dst_ref=side_ref.at[sub],
            send_sem=side_send.at[sub],
            recv_sem=side_recv.at[sub],
            device_id=to_side,
            device_id_type=MESH,
        )

    for step in range(zs):
        for way in range(2):
            core_copy(way, step).start()
    for step in range(zs):
        for sub in range(subs):
            for way in range(2):
                if sub == 0:
                    core_copy(way, step).wait_recv()
                piece = at(owner(way, step), way, core)
                span = pl.ds(sub * step_rows, step_rows)
                value = part_ref[piece, span, :].astype(jnp.float32) + core_ref[way, step, span, :].astype(jnp.float32)
                if step > 0:
                    ring_copy(way, step - 1, sub).wait_recv()
                    value = value + ring_ref[way, step - 1, sub].astype(jnp.float32)
                stage_ref[way, step, sub] = value.astype(stage_ref.dtype)
                if step < zs - 1:
                    ring_copy(way, step, sub).start()
        if step == zs - 1:
            for sub in range(subs):
                side_copy(sub).start()
    share = 1.0 / (4 * zs)
    for sub in range(subs):
        side_copy(sub).wait_recv()
        span = pl.ds(sub * step_rows, step_rows)
        total = stage_ref[xlo, zs - 1, sub].astype(jnp.float32) + side_ref[sub].astype(jnp.float32)
        out_ref[span, :] = total * share
    for step in range(zs):
        for way in range(2):
            core_copy(way, step).wait_send()
            for sub in range(subs):
                if step < zs - 1:
                    ring_copy(way, step, sub).wait_send()
    for sub in range(subs):
        side_copy(sub).wait_send()


def reduce_rows(part, dp_count, collective_id, subs=2):
    zs = dp_count // 4
    width = part.shape[1]
    rows = part.shape[0] // dp_count
    kind = part.dtype
    return pl.pallas_call(
        functools.partial(reduce_kernel, zs, subs),
        out_shape=jax.ShapeDtypeStruct((rows, width), jnp.float32),
        in_specs=[pl.BlockSpec(memory_space=pltpu.VMEM)],
        out_specs=pl.BlockSpec(memory_space=pltpu.VMEM),
        scratch_shapes=[
            pltpu.VMEM((2, zs, rows, width), kind),
            pltpu.VMEM((2, zs - 1, subs, rows // subs, width), kind),
            pltpu.VMEM((2, zs, subs, rows // subs, width), kind),
            pltpu.VMEM((subs, rows // subs, width), kind),
            pltpu.SemaphoreType.DMA((2, zs)),
            pltpu.SemaphoreType.DMA((2, zs)),
            pltpu.SemaphoreType.DMA((2, zs - 1, subs)),
            pltpu.SemaphoreType.DMA((2, zs - 1, subs)),
            pltpu.SemaphoreType.DMA((subs,)),
            pltpu.SemaphoreType.DMA((subs,)),
        ],
        compiler_params=pltpu.CompilerParams(
            collective_id=collective_id, has_side_effects=True, vmem_limit_bytes=32 * 1024 * 1024
        ),
        cost_estimate=pl.CostEstimate(flops=40_000_000_000, bytes_accessed=7_000_000, transcendentals=0),
        name="reduce_rows",
    )(part.reshape(dp_count, rows, width))


def gated_backward(gate_up, back_hidden):
    hidden = back_hidden.shape[1]
    gate_value = gate_up[:, :hidden]
    up_value = gate_up[:, hidden:]
    sigmoid_gate = jax.nn.sigmoid(gate_value)
    grad_gate = back_hidden * up_value * sigmoid_gate * (1.0 + gate_value * (1.0 - sigmoid_gate))
    grad_up = back_hidden * gate_value * sigmoid_gate
    return jnp.concatenate([grad_gate, grad_up], axis=1).astype(jnp.bfloat16)


def exchange(rows, experts, capacity):
    width = rows.shape[1]
    moved = lax.all_to_all(
        rows.reshape(experts, capacity, width), ROW_AXES, split_axis=0, concat_axis=0, tiled=True
    )
    return moved.reshape(experts * capacity, width)


def ring_offsets(zs):
    offsets = []
    for d in range(1, zs // 2):
        offsets += [-d, d]
    return offsets + [zs // 2, 0]


def near_slots(zs):
    return min(2, zs - 2)


def front_kernel(zs, xs, ys, capacity, stride, pieces, ids_ref, stash_ref, scale_ref, weight_ref, grad_ref,
                 rows_ref, plane_ref, picks_ref, slots_ref, tile_ref, near_ref, near_send, near_recv,
                 build_ref, build_sem, keep_sem, y_send, y_recv, x_send, x_recv, yx_send, yx_recv, xy_send, xy_recv):
    xlo, xhi, y = lax.axis_index("xlo"), lax.axis_index("xhi"), lax.axis_index("y")
    x = xhi * 2 + xlo
    z = lax.axis_index("z")
    tokens, width = stash_ref.shape
    depth = width // zs
    near = near_slots(zs)
    offsets = ring_offsets(zs)
    half = weight_ref.shape[0] // 2
    step = width // pieces

    def x_at(shift):
        return lax.rem(x + shift + xs, xs)

    def y_at(shift):
        return lax.rem(y + shift + ys, ys)

    def x_place(shift):
        return {"xlo": lax.rem(x_at(shift), 2), "xhi": x_at(shift) // 2}

    def y_place(shift):
        return {"y": y_at(shift)}

    def landed(xx, yy, part):
        return plane_ref.at[lax.rem(xx, 2), (xx // 2) * ys + yy, pl.ds(part * half, half), :]

    def moved(source, target, send, recv, device):
        return pltpu.make_async_remote_copy(
            src_ref=source, dst_ref=target, send_sem=send, recv_sem=recv, device_id=device, device_id_type=MESH
        )

    def z_at(slot):
        return lax.rem(z + offsets[slot] + zs, zs)

    greet(
        [x_place(k) for k in range(1, xs)]
        + [y_place(k) for k in range(1, ys)]
        + [{"z": z_at(slot)} for slot in range(near)]
    )
    own = [weight_ref.at[pl.ds(part * half, half), :] for part in range(2)]
    keep = pltpu.make_async_copy(weight_ref, plane_ref.at[xlo, xhi * ys + y], keep_sem)
    keep.start()
    sends, waits = [], []

    def send(copy):
        copy.start()
        sends.append(copy)

    for k in range(1, ys):
        send(moved(own[0], landed(x, y, 0), y_send.at[k - 1], y_recv.at[k - 1], y_place(k)))
    for k in range(1, xs):
        send(moved(own[1], landed(x, y, 1), x_send.at[k - 1], x_recv.at[k - 1], x_place(k)))
    for k in range(1, xs):
        send(moved(own[0], landed(x, y, 0), yx_send.at[0, k - 1], yx_recv.at[0, k - 1], x_place(k)))
    for k in range(1, ys):
        send(moved(own[1], landed(x, y, 1), xy_send.at[0, k - 1], xy_recv.at[0, k - 1], y_place(k)))

    for slot in range(near):
        columns = grad_ref.at[:, pl.ds(pl.multiple_of(z_at(slot) * depth, depth), depth)]
        send(moved(columns, near_ref.at[slot ^ 1], near_send.at[slot], near_recv.at[slot ^ 1], {"z": z_at(slot)}))

    expert = lax.broadcasted_iota(jnp.int32, tile_ref.shape, 0)
    first, second = ids_ref[0:1, :], ids_ref[1:2, :]
    tile_ref[...] = jnp.where(expert == 0, first, second)
    named = jnp.where((expert == first) | (expert == second), 1.0, 0.0).astype(jnp.bfloat16)
    ahead = jnp.where(
        lax.broadcasted_iota(jnp.int32, (tokens, tokens), 0) < lax.broadcasted_iota(jnp.int32, (tokens, tokens), 1),
        1.0, 0.0,
    ).astype(jnp.bfloat16)
    earlier = jnp.dot(named, ahead, preferred_element_type=jnp.float32)
    row = lax.broadcasted_iota(jnp.int32, (slots_ref.shape[0], tokens), 0).astype(jnp.float32)
    short = row[: rows_ref.shape[0]]
    hit = None
    for k, chosen in enumerate((first, second)):
        rank = jnp.sum(jnp.where(expert == chosen, earlier, 0.0), axis=0, keepdims=True)
        wide = row == chosen.astype(jnp.float32) * stride + rank
        slots_ref[:, k * tokens : (k + 1) * tokens] = jnp.where(wide, 1.0, 0.0).astype(slots_ref.dtype)
        match = short == chosen.astype(jnp.float32) * capacity + rank
        hit = match if hit is None else hit | match
    picks_ref[...] = jnp.where(hit, 1.0, 0.0).astype(picks_ref.dtype)
    blocks = scale_ref.shape[0]
    block = lax.broadcasted_iota(jnp.int32, (blocks, step), 0)
    lane = lax.broadcasted_iota(jnp.int32, (blocks, step), 1) // (width // blocks)
    per_step = step * blocks // width

    def build(piece, carry):
        spread = jnp.where(block == lane + piece * per_step, 1.0, 0.0).astype(jnp.bfloat16)
        scale = lax.dot_general(
            scale_ref[...], spread, (((0,), (0,)), ((), ())), preferred_element_type=jnp.float32
        )
        span = pl.ds(pl.multiple_of(piece * step, step), step)
        value = (stash_ref[:, span].astype(jnp.float32) * scale).astype(jnp.bfloat16)
        placed = jnp.dot(picks_ref[...], value, preferred_element_type=jnp.float32)
        build_ref[:, span] = placed.astype(build_ref.dtype)
        return carry

    lax.fori_loop(0, pieces // 4, build, 0)
    for j in range(1, ys):
        piece = landed(x, y_at(-j), 0)
        moved(own[0], piece, y_send.at[j - 1], y_recv.at[j - 1], y_place(j)).wait_recv()
        for k in range(1, xs):
            send(moved(piece, piece, yx_send.at[j, k - 1], yx_recv.at[j, k - 1], x_place(k)))
    for j in range(1, xs):
        piece = landed(x_at(-j), y, 1)
        moved(own[1], piece, x_send.at[j - 1], x_recv.at[j - 1], x_place(j)).wait_recv()
        for k in range(1, ys):
            send(moved(piece, piece, xy_send.at[j, k - 1], xy_recv.at[j, k - 1], y_place(k)))
    lax.fori_loop(pieces // 4, pieces, build, 0)
    put = pltpu.make_async_copy(build_ref, rows_ref, build_sem)
    put.start()
    for j in range(ys):
        for k in range(1, xs):
            piece = landed(x_at(-k), y_at(-j), 0)
            moved(own[0], piece, yx_send.at[j, k - 1], yx_recv.at[j, k - 1], x_place(k)).wait_recv()
    for j in range(xs):
        for k in range(1, ys):
            piece = landed(x_at(-j), y_at(-k), 1)
            moved(own[1], piece, xy_send.at[j, k - 1], xy_recv.at[j, k - 1], y_place(k)).wait_recv()
    for slot in range(near):
        landing = near_ref.at[slot]
        moved(landing, landing, near_send.at[slot], near_recv.at[slot], {"z": z_at(slot)}).wait_recv()
    for copy in sends:
        copy.wait_send()
    keep.wait()
    put.wait()


def front(id_rows, stash, scale_rows, w_down, out_grad, capacity, stride):
    tokens, width = stash.shape
    rows, hidden = w_down.shape
    experts = lax.axis_size(ROW_AXES)
    zs, xs, ys = lax.axis_size("z"), 2 * lax.axis_size("xhi"), lax.axis_size("y")
    near = near_slots(zs)
    kind = stash.dtype
    vmem = pl.BlockSpec(memory_space=pltpu.VMEM)
    anywhere = pl.BlockSpec(memory_space=pl.ANY)
    semaphores = []
    for shape in ((ys - 1,), (xs - 1,), (ys, xs - 1), (xs, ys - 1)):
        semaphores += [pltpu.SemaphoreType.DMA(shape), pltpu.SemaphoreType.DMA(shape)]
    return pl.pallas_call(
        functools.partial(front_kernel, zs, xs, ys, capacity, stride, 8),
        out_shape=(
            jax.ShapeDtypeStruct((experts * capacity, width), kind),
            jax.ShapeDtypeStruct((2, experts, rows, hidden), kind),
            jax.ShapeDtypeStruct((experts * capacity, tokens), kind),
            jax.ShapeDtypeStruct((experts * stride, 2 * tokens), kind),
            jax.ShapeDtypeStruct((8, tokens), id_rows.dtype),
            jax.ShapeDtypeStruct((near, tokens, width // zs), kind),
        ),
        in_specs=[vmem, vmem, vmem, vmem, anywhere],
        out_specs=(anywhere, anywhere, vmem, vmem, vmem, anywhere),
        scratch_shapes=[
            pltpu.SemaphoreType.DMA((near,)),
            pltpu.SemaphoreType.DMA((near,)),
            pltpu.VMEM((experts * capacity, width), kind),
            pltpu.SemaphoreType.DMA,
            pltpu.SemaphoreType.DMA,
        ] + semaphores,
        compiler_params=pltpu.CompilerParams(
            collective_id=3, has_side_effects=True, vmem_limit_bytes=60 * 1024 * 1024
        ),
        cost_estimate=pl.CostEstimate(flops=20_000_000_000, bytes_accessed=10_000_000, transcendentals=0),
        name="front",
    )(id_rows, stash, scale_rows, w_down, out_grad)


def relay_kernel(zs, grad_ref, near_ref, ids_in_ref, gate_ref, weight_ref, slots_ref, out_ref, ids_ref, turn_ref, ids_send, ids_recv,
                 tail_ref, tail_send, tail_recv, tail_sem, slice_ref, wide_ref, pick_ref, stage_ref, back_ref,
                 own_sem, near_sem, slice_send, slice_recv, weight_sem, weight_send, weight_recv, back_send, back_recv):
    z, xlo, core = ring_place()
    tokens = slice_ref.shape[1]
    depth = slice_ref.shape[2]
    experts_out = out_ref.shape[0]
    mine = lax.axis_index("xhi") * (experts_out // 2) + lax.axis_index("y")

    def row_of(shift):
        return lax.rem(mine + shift, experts_out)

    def row_place(shift):
        row = row_of(shift)
        return {"xhi": row // (experts_out // 2), "y": lax.rem(row, experts_out // 2)}

    experts = weight_ref.shape[1]
    rows = weight_ref.shape[2]
    half = zs // 2
    offsets = ring_offsets(zs)
    near = near_slots(zs)
    twin = place(z, xlo, 1 - core)

    def peer(offset):
        return lax.rem(z + offset + zs, zs)

    def mirror(slot):
        return slot if slot >= zs - 2 else slot ^ 1

    greet(
        [place(peer(offset), xlo, core) for offset in offsets[:-1]]
        + [twin]
        + [row_place(shift) for shift in range(1, experts_out)]
    )

    def tail_copy(shift):
        return pltpu.make_async_remote_copy(
            src_ref=tail_ref.at[row_of(shift)],
            dst_ref=out_ref.at[mine],
            send_sem=tail_send.at[shift - 1],
            recv_sem=tail_recv.at[shift - 1],
            device_id=row_place(shift),
            device_id_type=MESH,
        )

    def tail_arrival(shift):
        source = row_of(experts_out - shift)
        return pltpu.make_async_remote_copy(
            src_ref=tail_ref.at[source],
            dst_ref=out_ref.at[source],
            send_sem=tail_send.at[shift - 1],
            recv_sem=tail_recv.at[shift - 1],
            device_id=twin,
            device_id_type=MESH,
        )

    def ids_copy(slot):
        return pltpu.make_async_remote_copy(
            src_ref=ids_in_ref,
            dst_ref=ids_ref.at[mirror(slot)],
            send_sem=ids_send.at[slot],
            recv_sem=ids_recv.at[mirror(slot)],
            device_id=place(peer(offsets[slot]), xlo, core),
            device_id_type=MESH,
        )

    def ids_arrival(slot):
        return pltpu.make_async_remote_copy(
            src_ref=ids_ref.at[slot],
            dst_ref=ids_ref.at[slot],
            send_sem=ids_send.at[slot],
            recv_sem=ids_recv.at[slot],
            device_id=twin,
            device_id_type=MESH,
        )

    def columns(offset):
        return pl.ds(pl.multiple_of(peer(offset) * depth, depth), depth)

    def slice_copy(slot):
        return pltpu.make_async_remote_copy(
            src_ref=grad_ref.at[:, columns(offsets[slot])],
            dst_ref=slice_ref.at[mirror(slot)],
            send_sem=slice_send.at[slot],
            recv_sem=slice_recv.at[mirror(slot)],
            device_id=place(peer(offsets[slot]), xlo, core),
            device_id_type=MESH,
        )

    def back_copy(slot):
        return pltpu.make_async_remote_copy(
            src_ref=stage_ref.at[slot],
            dst_ref=back_ref.at[mirror(slot)],
            send_sem=back_send.at[slot],
            recv_sem=back_recv.at[mirror(slot)],
            device_id=place(peer(offsets[slot]), xlo, core),
            device_id_type=MESH,
        )

    def slice_arrival(slot):
        return pltpu.make_async_remote_copy(
            src_ref=slice_ref.at[slot],
            dst_ref=slice_ref.at[slot],
            send_sem=slice_send.at[slot],
            recv_sem=slice_recv.at[slot],
            device_id=twin,
            device_id_type=MESH,
        )

    def back_arrival(slot):
        return pltpu.make_async_remote_copy(
            src_ref=back_ref.at[slot],
            dst_ref=back_ref.at[slot],
            send_sem=back_send.at[slot],
            recv_sem=back_recv.at[slot],
            device_id=twin,
            device_id_type=MESH,
        )

    def weight_rows(plane, side):
        return wide_ref.at[:, pl.ds(pl.multiple_of((2 * plane + side) * rows, rows), rows), :]

    def weight_copy(plane):
        return pltpu.make_async_remote_copy(
            src_ref=weight_ref.at[plane],
            dst_ref=weight_rows(plane, core),
            send_sem=weight_send.at[plane],
            recv_sem=weight_recv.at[plane],
            device_id=twin,
            device_id_type=MESH,
        )

    def weight_arrival(plane):
        return pltpu.make_async_remote_copy(
            src_ref=weight_ref.at[plane],
            dst_ref=weight_rows(plane, 1 - core),
            send_sem=weight_send.at[plane],
            recv_sem=weight_recv.at[plane],
            device_id=twin,
            device_id_type=MESH,
        )

    keeps = [pltpu.make_async_copy(grad_ref.at[:, columns(0)], slice_ref.at[zs - 1], own_sem)]
    keeps.append(pltpu.make_async_copy(near_ref, slice_ref.at[pl.ds(0, near)], near_sem))
    for plane in range(2):
        keeps.append(pltpu.make_async_copy(weight_ref.at[plane], weight_rows(plane, core), weight_sem.at[plane]))
    for slot in range(zs - 1):
        ids_copy(slot).start()
    for slot in range(near, zs - 1):
        slice_copy(slot).start()
    for plane in range(2):
        weight_copy(plane).start()
    ids_ref[zs - 1] = ids_in_ref[...]
    for keep in keeps:
        keep.start()
    for keep in keeps:
        keep.wait()
    for plane in range(2):
        weight_arrival(plane).wait_recv()
    for pair in range(half):
        for side in range(2):
            slot = 2 * pair + side
            if slot < zs - 1:
                ids_arrival(slot).wait_recv()
                if slot >= near:
                    slice_arrival(slot).wait_recv()
        pick_ref[...] = jnp.zeros_like(pick_ref)
        for side in range(2):
            tall = jnp.concatenate([ids_ref[2 * pair + side]] * (tokens // ids_ref.shape[1]), axis=0)
            turn_ref[pl.ds(side * tokens, tokens), :] = tall.T

        def per_expert(e, carry):
            both = slice_ref[pl.ds(2 * pair, 2)].reshape(2 * tokens, depth)
            dense = jnp.dot(both, wide_ref[e], preferred_element_type=jnp.float32)
            for k in range(2):
                pick_ref[k] = jnp.where(turn_ref[:, k : k + 1] == e, dense, pick_ref[k])
            return carry

        lax.fori_loop(0, experts, per_expert, 0)
        for side in range(2):
            slot = 2 * pair + side
            for k in range(2):
                stage_ref[slot, k] = pick_ref[k, pl.ds(side * tokens, tokens), :].astype(stage_ref.dtype)
            if slot < zs - 1:
                back_copy(slot).start()
    total = stage_ref[zs - 1].astype(jnp.float32)
    for slot in range(zs - 1):
        back_arrival(slot).wait_recv()
        total = total + back_ref[slot].astype(jnp.float32)
    weighted = [(total[k] * gate_ref[:, k : k + 1]).astype(tail_ref.dtype) for k in range(2)]
    placed = jnp.dot(slots_ref[...], jnp.concatenate(weighted, axis=0), preferred_element_type=jnp.float32)
    tail_ref[...] = placed.astype(tail_ref.dtype).reshape(tail_ref.shape)
    for shift in range(1, experts_out):
        tail_copy(shift).start()
    keep_tail = pltpu.make_async_copy(tail_ref.at[mine], out_ref.at[mine], tail_sem)
    keep_tail.start()
    for slot in range(zs - 1):
        ids_copy(slot).wait_send()
        if slot >= near:
            slice_copy(slot).wait_send()
        back_copy(slot).wait_send()
    for plane in range(2):
        weight_copy(plane).wait_send()
    for shift in range(1, experts_out):
        tail_arrival(shift).wait_recv()
        tail_copy(shift).wait_send()
    keep_tail.wait()


def relay(out_grad, near, route_ids, gates, weights, slots, zs):
    tokens, feature_width = out_grad.shape
    planes, experts, rows, hidden = weights.shape
    depth = feature_width // zs
    tail_rows = slots.shape[0] // experts
    kind = out_grad.dtype
    vmem = pl.BlockSpec(memory_space=pltpu.VMEM)
    anywhere = pl.BlockSpec(memory_space=pl.ANY)
    pairs = pltpu.SemaphoreType.DMA((zs - 1,))
    others = pltpu.SemaphoreType.DMA((experts - 1,))
    return pl.pallas_call(
        functools.partial(relay_kernel, zs),
        out_shape=jax.ShapeDtypeStruct((experts, tail_rows, hidden), kind),
        in_specs=[anywhere, anywhere, vmem, vmem, anywhere, vmem],
        out_specs=anywhere,
        scratch_shapes=[
            pltpu.VMEM((zs,) + route_ids.shape, route_ids.dtype),
            pltpu.VMEM((2 * tokens, tokens), route_ids.dtype),
            pairs,
            pairs,
            pltpu.VMEM((experts, tail_rows, hidden), kind),
            others,
            others,
            pltpu.SemaphoreType.DMA,
            pltpu.VMEM((zs, tokens, depth), kind),
            pltpu.VMEM((experts, 2 * planes * rows, hidden), kind),
            pltpu.VMEM((2, 2 * tokens, hidden), jnp.float32),
            pltpu.VMEM((zs, 2, tokens, hidden), kind),
            pltpu.VMEM((zs - 1, 2, tokens, hidden), kind),
            pltpu.SemaphoreType.DMA,
            pltpu.SemaphoreType.DMA,
            pairs,
            pairs,
            pltpu.SemaphoreType.DMA((2,)),
            pltpu.SemaphoreType.DMA((2,)),
            pltpu.SemaphoreType.DMA((2,)),
            pairs,
            pairs,
        ],
        compiler_params=pltpu.CompilerParams(
            collective_id=1, has_side_effects=True, vmem_limit_bytes=24 * 1024 * 1024
        ),
        cost_estimate=pl.CostEstimate(flops=40_000_000_000, bytes_accessed=7_000_000, transcendentals=0),
        name="relay",
    )(out_grad, near, route_ids, gates, weights, slots)


def on_device(stash, scales, out_grad, route_ids, gates, w_gate_up, w_down):
    tokens, feature_width = stash.shape
    hidden = w_down.shape[2]
    experts = lax.axis_size(ROW_AXES)
    dp_count = lax.axis_size(COLUMN_AXES)
    capacity = min(tokens, 7 * tokens // (2 * experts))
    stride = -(-capacity // 16) * 16
    sent_x, weights, picks, slots, id_rows, near = front(
        route_ids.T, stash, scales.T, w_down[0], out_grad, capacity, stride
    )
    weight_in = w_gate_up[0]
    zs = lax.axis_size("z")
    features = exchange(sent_x, experts, capacity)
    got_hidden = relay(out_grad, near, id_rows, gates, weights, slots, zs)
    back_hidden = got_hidden[:, :capacity].reshape(experts * capacity, hidden).astype(jnp.float32)
    gate_up = jnp.dot(features, weight_in, preferred_element_type=jnp.float32)
    hidden_grad = gated_backward(gate_up, back_hidden)
    slot_grads = lax.dot_general(
        hidden_grad, weight_in, (((1,), (1,)), ((), ())), preferred_element_type=jnp.float32
    ).astype(jnp.bfloat16)
    returned = exchange(slot_grads, experts, capacity)
    input_grad = lax.dot_general(
        picks, returned, (((0,), (0,)), ((), ())), preferred_element_type=jnp.float32
    ).astype(jnp.bfloat16)
    local_rows = feature_width // dp_count
    partial_grad = lax.dot_general(
        features, hidden_grad, (((0,), (0,)), ((), ())), preferred_element_type=jnp.float32
    ).astype(jnp.bfloat16)
    grad_gate_up = reduce_rows(partial_grad, dp_count, 2).reshape(1, local_rows, 2 * hidden)
    return (input_grad, grad_gate_up)


def solution(mesh):
    dp_count, experts = mesh.devices.shape
    split = Mesh(
        mesh.devices.reshape(dp_count // 4, 2, 2, 2, experts // 2), COLUMN_AXES + ROW_AXES
    )
    tokens = P(COLUMN_AXES + ROW_AXES, None)
    placed = (tokens, tokens, tokens, tokens, tokens, P(ROW_AXES, None, None), P(ROW_AXES, COLUMN_AXES, None))
    return jax.shard_map(
        on_device,
        mesh=split,
        in_specs=placed,
        out_specs=(tokens, P(ROW_AXES, COLUMN_AXES, None)),
        check_vma=False,
    )
```
